256 devices in a mesh: rep: 2 (over core), dp: 128 (over x, y, z).
Axes of the slice: x: 4, y: 4, z: 8, core: 2. Of those that a mesh axis runs over, the one named last changes fastest.
Arguments:
- x: bfloat16 [256, 2048, 512], P(('rep', 'dp')), parts along dimension 0
- dy: bfloat16 [256, 2048, 512], P(('rep', 'dp')), parts along dimension 0
- w_gate: bfloat16 [2, 512, 1536], replicated
- w_up: bfloat16 [2, 512, 1536], replicated
- w_down: bfloat16 [2, 1536, 512], replicated
- m_w_gate: float32 [2, 512, 1536], replicated
- m_w_up: float32 [2, 512, 1536], replicated
- m_w_down: float32 [2, 1536, 512], replicated
- v_w_gate: float32 [2, 512, 1536], replicated
- v_w_up: float32 [2, 512, 1536], replicated
- v_w_down: float32 [2, 1536, 512], replicated
Outputs:
- output 1: bfloat16 [4, 512, 1536], P('rep'), parts along dimension 0
- output 2: bfloat16 [4, 512, 1536], P('rep'), parts along dimension 0
- output 3: bfloat16 [4, 1536, 512], P('rep'), parts along dimension 0
- output 4: float32 [4, 512, 1536], P('rep'), parts along dimension 0
- output 5: float32 [4, 512, 1536], P('rep'), parts along dimension 0
- output 6: float32 [4, 1536, 512], P('rep'), parts along dimension 0
- output 7: float32 [4, 512, 1536], P('rep'), parts along dimension 0
- output 8: float32 [4, 512, 1536], P('rep'), parts along dimension 0
- output 9: float32 [4, 1536, 512], P('rep'), parts along dimension 0
There are 2 independent parts. The reference program is written for one: setup_inputs(seed, part) draws one part's arguments, and reference() takes and returns one part's arrays. A program takes and returns all parts, laid end to end along the dimension named above; an argument that names none is the same for every part.
All inputs are finite; a program needn't handle non-finite values.
Results may differ from the reference program's by a relative error of at most 0.022.
Values are sent between devices in bfloat16 or wider.
A program may use at most 768 MiB of HBM per device.

```python
import jax
import jax.numpy as jnp
from jax import lax

SEQUENCES = 128
TOKENS = 2048
D = 512
FF = 1536
LAYERS = 2
NAMES = ("w_gate", "w_up", "w_down")
SHAPES = {"w_gate": (LAYERS, D, FF), "w_up": (LAYERS, D, FF), "w_down": (LAYERS, FF, D)}


def bump(key, n, height):
    away = (jnp.arange(n, dtype=jnp.int32) - jax.random.randint(key, (), 0, n, jnp.int32)) % n
    return jnp.where(away < n // 8, height, 1.0)


def together(key, own, strength):
    shared = jax.random.normal(key, own.shape[1:], jnp.float32)
    return (own + strength * shared) * lax.rsqrt(1 + strength * strength)


def setup_inputs(seed: int = 0, part: int = 0) -> dict:
    kx, kdy, ka, kb, kz, kf, kh, kl, *keys = jax.random.split(jax.random.key(seed), 8 + 3 * len(NAMES))
    kx, kdy, ka, kb = (jax.random.fold_in(k, part) for k in (kx, kdy, ka, kb))
    kw, km, kv = (keys[i::3] for i in range(3))
    shape = (SEQUENCES, TOKENS, D)
    much_x, much_dy = jax.random.uniform(kz, (2,), jnp.float32, 0.0, 1.0)
    loud = 2.0 ** jax.random.uniform(jax.random.fold_in(kz, 1), (), jnp.float32, -1.0, 2.0)
    layers = 2.0 ** jax.random.uniform(kl, (LAYERS, 1, 1), jnp.float32, -1.0, 1.0)
    x = together(ka, jax.random.normal(kx, shape, jnp.float32), much_x) * bump(kf, D, 4.0)
    dy = together(kb, jax.random.normal(kdy, shape, jnp.float32), much_dy)
    drawn = {"x": x.astype(jnp.bfloat16), "dy": (loud * dy * (SEQUENCES * TOKENS) ** -0.5).astype(jnp.bfloat16)}
    for key, name in zip(kw, NAMES, strict=True):
        w = jax.random.normal(key, SHAPES[name], jnp.float32) * SHAPES[name][1] ** -0.5
        drawn[name] = (w * {"w_gate": 1.0, "w_up": bump(kh, FF, 4.0), "w_down": layers}[name]).astype(jnp.bfloat16)
    for key, name in zip(km, NAMES, strict=True):
        drawn[f"m_{name}"] = 0.1 * jax.random.normal(key, SHAPES[name], jnp.float32)
    for key, name in zip(kv, NAMES, strict=True):
        drawn[f"v_{name}"] = loud * loud * jax.random.uniform(key, SHAPES[name], jnp.float32, 0.05, 0.15)
    return drawn


def matmul(a, w):
    return jnp.dot(a, w, preferred_element_type=jnp.float32).astype(jnp.bfloat16)


def normed(h):
    wide = h.astype(jnp.float32)
    scale = lax.rsqrt(jnp.mean(wide**2, -1, keepdims=True) + 1e-6)
    return (wide * scale).astype(jnp.bfloat16)


def layer(h, w):
    a = normed(h)
    gate = jnp.dot(a, w["w_gate"], preferred_element_type=jnp.float32)
    up = jnp.dot(a, w["w_up"], preferred_element_type=jnp.float32)
    return h + matmul((jax.nn.silu(gate) * up).astype(jnp.bfloat16), w["w_down"])


def adamw(w, m, v, g):
    m = 0.9 * m + 0.1 * g
    v = 0.95 * v + 0.05 * g * g
    step = m * lax.rsqrt(v + 1e-8) + 0.1 * w
    return (w - 0.02 * step).astype(jnp.bfloat16), m, v


def stack(weights, h):
    return lax.scan(lambda h, w: (layer(h, w), None), h, weights)[0]


def reference(x, dy, w_gate, w_up, w_down, m_w_gate, m_w_up, m_w_down, v_w_gate, v_w_up, v_w_down):
    weights = dict(zip(NAMES, (w_gate, w_up, w_down), strict=True))

    def take(so_far, sequence):
        h, by_y = sequence
        _, back = jax.vjp(lambda w: stack(w, h), weights)
        return jax.tree.map(lambda total, term: total + term.astype(jnp.float32), so_far, back(by_y)[0]), None

    none_yet = {name: jnp.zeros(w.shape, jnp.float32) for name, w in weights.items()}
    by_weights, _ = lax.scan(take, none_yet, (x, dy))
    gradients = [by_weights[name].astype(jnp.bfloat16).astype(jnp.float32) for name in NAMES]
    new = [
        adamw(w.astype(jnp.float32), m, v, g)
        for w, m, v, g in zip((w_gate, w_up, w_down), (m_w_gate, m_w_up, m_w_down), (v_w_gate, v_w_up, v_w_down), gradients, strict=True)
    ]
    return tuple(one[which] for which in range(3) for one in new)
```

```python
import functools

import jax
import jax.numpy as jnp
from jax import lax
from jax.experimental import pallas as pl
from jax.experimental.pallas import tpu as pltpu
from jax.sharding import PartitionSpec as P

NAMES = ("w_gate", "w_up", "w_down")
MESH = pl.DeviceIdType.MESH
DIMS = (4, 4, 8)
BLOCK = 512
TICKS = 3
BF16, F32 = jnp.bfloat16, jnp.float32


def matmul(a, w):
    return jnp.dot(a, w, preferred_element_type=jnp.float32).astype(jnp.bfloat16)


def normed(h):
    wide = h.astype(jnp.float32)
    scale = lax.rsqrt(jnp.mean(wide**2, -1, keepdims=True) + 1e-6)
    return (wide * scale).astype(jnp.bfloat16)


def layer(h, w):
    a = normed(h)
    gate = jnp.dot(a, w["w_gate"], preferred_element_type=jnp.float32)
    up = jnp.dot(a, w["w_up"], preferred_element_type=jnp.float32)
    return h + matmul((jax.nn.silu(gate) * up).astype(jnp.bfloat16), w["w_down"])


def adamw(w, m, v, g):
    m = 0.9 * m + 0.1 * g
    v = 0.95 * v + 0.05 * g * g
    step = m * lax.rsqrt(v + 1e-8) + 0.1 * w
    return (w - 0.02 * step).astype(jnp.bfloat16), m, v


def ds(start, size, multiple=None):
    if isinstance(start, int):
        return pl.ds(start, size)
    return pl.ds(pl.multiple_of(start, multiple or size), size)


class Torus:
    def __init__(self):
        i = lax.axis_index("dp")
        nx, ny, nz = DIMS
        self.at = (lax.div(i, ny * nz), lax.rem(lax.div(i, nz), ny), lax.rem(i, nz))

    def shifted(self, axis, by):
        n = DIMS[axis]
        return lax.rem(self.at[axis] + (by % n), n)

    def device(self, axis, by):
        to = list(self.at)
        to[axis] = self.shifted(axis, by)
        return {"dp": (to[0] * DIMS[1] + to[1]) * DIMS[2] + to[2]}

    def barrier(self):
        sem = pltpu.get_barrier_semaphore()
        peers = [(axis, by) for axis in range(3) for by in range(1, DIMS[axis])]
        for axis, by in peers:
            pl.semaphore_signal(sem, inc=1, device_id=self.device(axis, by), device_id_type=MESH)
        pl.semaphore_wait(sem, len(peers))


class Step:
    def __init__(self, start, finish):
        self.start, self.finish = start, finish


def rows_loop(rows, lanes, body):
    size = min(rows, max(16, 16 * (512 // lanes)))
    if rows == size:
        body(0, size)
        return

    def one(i, _):
        body(pl.multiple_of(i * size, size), size)
        return 0

    lax.fori_loop(0, rows // size, one, 0)


class Exchange:
    def __init__(self, torus, order, chained, chunk, rx, p32, pb, r32, rb, sems, sites):
        self.torus, self.order, self.chained = torus, order, chained
        self.chunk = chunk
        self.rx1, self.rx2, self.rx3 = rx
        self.p32, self.pb, self.r32, self.rb = p32, pb, r32, rb
        self.send_sems, self.recv_sems = sems
        self.sites = sites
        n1, n2, n3 = (DIMS[a] for a in order)
        self.rows1 = BLOCK // n1
        self.lanes2 = BLOCK // n2
        self.rows3 = self.rows1 // n3
        self.steps = self._steps()

    def _site(self):
        s = self.sites[0]
        self.sites[0] += 1
        return s

    def _copy(self, c, site, src, dst, axis, by):
        slot = c
        pltpu.make_async_remote_copy(
            src_ref=src,
            dst_ref=dst,
            send_sem=self.send_sems.at[slot, site],
            recv_sem=self.recv_sems.at[slot, site],
            device_id=self.torus.device(axis, by),
            device_id_type=MESH,
        ).start()

    def _wait(self, c, site, like, recv):
        sem = (self.recv_sems if recv else self.send_sems).at[c, site]
        pltpu.make_async_copy(like, like, sem).wait()

    def _chain(self, axis, rows, lanes, send_ref, own, rx, total):
        n = DIMS[axis]
        k = n // 2
        half = rows // 2
        ways = ((1, 0, 0), (-1, 1, half))
        steps = []
        for s in range(1, k + 1):
            sites = [self._site() for _ in ways]

            def start(c, s=s, sites=sites):
                for (way, w, h0), site in zip(ways, sites, strict=True):
                    t = self.torus.shifted(axis, way * (k + 1 - s))
                    dst = rx(c, w, s - 1)
                    if s == 1:
                        self._copy(c, site, send_ref(c, t, h0, half), dst.at[ds(h0, half), :], axis, way)
                    elif s == 2:
                        o0 = half - h0
                        self._copy(c, site, rx(c, w, 0).at[ds(h0, half), :], dst.at[ds(h0, half), :], axis, way)
                        self._copy(c, site, send_ref(c, t, o0, half), dst.at[ds(o0, half), :], axis, way)
                    else:
                        self._copy(c, site, rx(c, w, s - 2), dst, axis, way)

            def finish(c, s=s, sites=sites):
                for (way, w, h0), site in zip(ways, sites, strict=True):
                    got = rx(c, w, s - 1)
                    part = got.at[ds(h0, half), :] if s == 1 else got
                    self._wait(c, site, part, True)
                    if s < k:
                        t = self.torus.shifted(axis, way * (k - s))
                        first, count = (h0, half) if s == 1 else (0, rows)

                        def add(r0, size, got=got, t=t, first=first):
                            at = ds(first + r0, size, 16)
                            got[at, :] = (got[at, :].astype(F32) + own(c, t, first + r0, size)).astype(BF16)

                        rows_loop(count, lanes, add)
                if s == k:
                    me = self.torus.shifted(axis, 0)
                    for first in (0, half):

                        def add(r0, size, first=first):
                            at = ds(first + r0, size, 16)
                            value = own(c, me, first + r0, size)
                            for way, w, h0 in ways:
                                if k > 1 or h0 == first:
                                    value = value + rx(c, w, k - 1)[at, :].astype(F32)
                            total(c, first + r0, size, value)

                        rows_loop(half, lanes, add)
                for (way, w, h0), site in zip(ways, sites, strict=True):
                    got = rx(c, w, s - 1)
                    self._wait(c, site, got.at[ds(h0, half), :] if s == 1 else got, False)

            steps.append(Step(start, finish))
        return steps

    def _chain_gather(self, axis, rows, block):
        n = DIMS[axis]
        k = n // 2
        half = rows // 2
        ways = ((1, 0), (-1, half))
        steps = []
        for s in range(1, k + 1):
            sites = [self._site() for _ in ways]

            def start(c, s=s, sites=sites):
                for (way, h0), site in zip(ways, sites, strict=True):
                    t = self.torus.shifted(axis, -way * (s - 1))
                    ref = block(c, t, h0, half) if s == k else block(c, t, 0, rows)
                    self._copy(c, site, ref, ref, axis, way)

            def finish(c, s=s, sites=sites):
                for recv in (True, False):
                    for (way, h0), site in zip(ways, sites, strict=True):
                        t = self.torus.shifted(axis, -way * s)
                        self._wait(c, site, block(c, t, h0, half) if s == k else block(c, t, 0, rows), recv)

            steps.append(Step(start, finish))
        return steps

    def _direct(self, axis, rows, lanes, send_ref, own, rx, total):
        n = DIMS[axis]
        site = self._site()

        def start(c):
            for by in range(1, n):
                t = self.torus.shifted(axis, by)
                self._copy(c, site, send_ref(c, t), rx(c).at[by - 1], axis, by)

        def finish(c):
            self._wait(c, site, rx(c), True)

            def add(r0, size):
                value = own(c, r0, size)
                for i in range(n - 1):
                    value = value + rx(c)[i, ds(r0, size, 16), :].astype(F32)
                total(c, r0, size, value)

            rows_loop(rows, lanes, add)
            self._wait(c, site, rx(c), False)

        return [Step(start, finish)]

    def _direct_gather(self, axis, mine, like):
        n = DIMS[axis]
        site = self._site()

        def start(c):
            for by in range(1, n):
                self._copy(c, site, mine(c), mine(c), axis, by)

        def finish(c):
            self._wait(c, site, like(c), True)
            self._wait(c, site, like(c), False)

        return [Step(start, finish)]

    def _steps(self):
        a1, a2, a3 = self.order
        rows1, lanes2, rows3 = self.rows1, self.lanes2, self.rows3
        at = [self.torus.at[a] for a in self.order]
        chunk = self.chunk

        def block1(c, t, r0, n):
            return chunk(c).at[ds(t * rows1 + r0, n, 16), :]

        def own1(c, t, r0, n):
            return chunk(c)[ds(t * rows1 + r0, n, 16), :].astype(F32)

        def total1(c, r0, n, value):
            at_ = ds(r0, n, 16)
            self.p32[c % 2, at_, :] = value
            self.pb[c % 2, at_, :] = value.astype(BF16)

        steps = self._chain(a1, rows1, BLOCK, block1, own1, lambda c, w, s: self.rx1.at[c, w, s], total1)

        def own2(c, t, r0, n):
            return self.p32[c % 2, ds(r0, n, 16), ds(t * lanes2, lanes2)]

        def total2(c, r0, n, value):
            at_ = ds(r0, n, 16)
            self.r32[c % 2, at_, :] = value
            self.rb[c % 2, at_, :] = value.astype(BF16)

        if self.chained:
            steps += self._chain(
                a2,
                rows1,
                lanes2,
                lambda c, t, r0, n: self.pb.at[c % 2, ds(r0, n, 16), ds(t * lanes2, lanes2)],
                own2,
                lambda c, w, s: self.rx2.at[c, w, s],
                total2,
            )
        else:
            steps += self._direct(
                a2,
                rows1,
                lanes2,
                lambda c, t: self.pb.at[c % 2, :, ds(t * lanes2, lanes2)],
                lambda c, r0, n: own2(c, at[1], r0, n),
                lambda c: self.rx2.at[c],
                total2,
            )

        def final(c):
            return chunk(c).at[ds(at[0] * rows1 + at[2] * rows3, rows3, 16), ds(at[1] * lanes2, lanes2)]

        def total3(c, r0, n, value):
            final(c)[ds(r0, n, 16), :] = value.astype(BF16)

        steps += self._direct(
            a3,
            rows3,
            lanes2,
            lambda c, t: self.rb.at[c % 2, ds(t * rows3, rows3, 16), :],
            lambda c, r0, n: self.r32[c % 2, ds(at[2] * rows3 + r0, n, 16), :],
            lambda c: self.rx3.at[c],
            total3,
        )
        steps += self._direct_gather(a3, final, lambda c: self.rx3.at[c])

        def block2(c, t, r0, n):
            return chunk(c).at[ds(at[0] * rows1 + r0, n, 16), ds(t * lanes2, lanes2)]

        if self.chained:
            steps += self._chain_gather(a2, rows1, block2)
        else:
            steps += self._direct_gather(a2, lambda c: block2(c, at[1], 0, rows1), lambda c: self.rx2.at[c])
        steps += self._chain_gather(a1, rows1, block1)
        return steps

    @staticmethod
    def scratch(order, chained, chunks):
        n1, n2, n3 = (DIMS[a] for a in order)
        rows1, lanes2 = BLOCK // n1, BLOCK // n2
        rx2 = (chunks, 2, n2 // 2, rows1, lanes2) if chained else (chunks, n2 - 1, rows1, lanes2)
        return [
            pltpu.VMEM((chunks, 2, n1 // 2, rows1, BLOCK), BF16),
            pltpu.VMEM(rx2, BF16),
            pltpu.VMEM((chunks, n3 - 1, rows1 // n3, lanes2), BF16),
            pltpu.VMEM((2, rows1, BLOCK), F32),
            pltpu.VMEM((2, rows1, BLOCK), BF16),
            pltpu.VMEM((2, rows1, lanes2), F32),
            pltpu.VMEM((2, rows1, lanes2), BF16),
        ]

    @staticmethod
    def n_sites(order, chained):
        k1, k2 = DIMS[order[0]] // 2, DIMS[order[1]] // 2
        return 4 * k1 + (4 * k2 if chained else 2) + 2


COLOURS = (((0, 1, 2), True), ((1, 0, 2), True), ((2, 0, 1), False))


def tick(exchanges, c_of, s, period):
    longest = max(len(e.steps) for e in exchanges)
    for late in range(s, longest + 1, TICKS):
        c = period - late // TICKS
        done = late

        @pl.when((c >= 0) & (c < c_of))
        def _(c=c, done=done):
            for e in exchanges:
                if 1 <= done <= len(e.steps):
                    e.steps[done - 1].finish(c)
            for e in exchanges:
                if done < len(e.steps):
                    e.steps[done].start(c)


def exchange_kernel(chunks, g_down, g_gate, g_up, o_down, o_gate, o_up, g, *scratch):
    torus = Torus()
    per = len(scratch) - 3
    send_sems, recv_sems, io_sems = scratch[per:]
    blocks = g_gate.shape[2] // BLOCK

    def io(c, colour, down, gate, up):
        number, j = 1 - lax.div(c, blocks), lax.rem(c, blocks)
        if colour == 0:
            return down.at[number, ds(j * BLOCK, BLOCK), :]
        return (gate, up)[colour - 1].at[number, :, ds(j * BLOCK, BLOCK)]

    def load(c):
        return [pltpu.make_async_copy(io(c, k, g_down, g_gate, g_up), g.at[c, k], io_sems.at[c, k]) for k in range(3)]

    def save(c):
        return [pltpu.make_async_copy(g.at[c, k], io(c, k, o_down, o_gate, o_up), io_sems.at[c, k]) for k in range(3)]

    for c in range(chunks):
        for copy in load(c):
            copy.start()
    torus.barrier()
    sites = [0]
    exchanges = []
    for k, (order, chained) in enumerate(COLOURS):
        rx = scratch[7 * k : 7 * k + 3]
        exchanges.append(
            Exchange(torus, order, chained, lambda c, k=k: g.at[c, k], rx, *scratch[7 * k + 3 : 7 * k + 7], (send_sems, recv_sems), sites)
        )
    longest = max(len(e.steps) for e in exchanges)
    last = longest // TICKS
    ready = longest % TICKS

    def body(period, _):
        @pl.when(period < chunks)
        def _():
            for copy in load(period):
                copy.wait()

        for s in range(TICKS):
            tick(exchanges, chunks, s, period)
            if s == ready:
                c = period - last

                @pl.when((c >= 0) & (c < chunks))
                def _():
                    for copy in save(c):
                        copy.start()

        return 0

    lax.fori_loop(0, chunks + last, body, 0)
    for c in range(chunks):
        for copy in save(c):
            copy.wait()


def exchange(down, gate, up):
    chunks = gate.shape[0] * gate.shape[2] // BLOCK
    scratch, n_sites = [pltpu.VMEM((chunks, 3, BLOCK, BLOCK), BF16)], 0
    for order, chained in COLOURS:
        scratch += Exchange.scratch(order, chained, chunks)
        n_sites += Exchange.n_sites(order, chained)
    scratch += [pltpu.SemaphoreType.DMA((chunks, n_sites))] * 2 + [pltpu.SemaphoreType.DMA((chunks, 3))]
    return pl.pallas_call(
        functools.partial(exchange_kernel, chunks),
        out_shape=[jax.ShapeDtypeStruct(a.shape, a.dtype) for a in (down, gate, up)],
        in_specs=[pl.BlockSpec(memory_space=pl.ANY)] * 3,
        out_specs=[pl.BlockSpec(memory_space=pl.ANY)] * 3,
        scratch_shapes=scratch,
        compiler_params=pltpu.CompilerParams(collective_id=0, has_side_effects=True, vmem_limit_bytes=60 << 20),
        name="exchange",
    )(down, gate, up)


def solution(mesh):
    def step(x, dy, *arrays):
        weights, m, v = (arrays[i : i + 3] for i in (0, 3, 6))
        layers = weights[0].shape[0]
        h, kept = x[0], []
        for number in range(layers):
            kept.append(h)
            h = layer(h, {name: w[number] for name, w in zip(NAMES, weights, strict=True)})
        by_h, own = dy[0], [None] * layers
        for number in reversed(range(layers)):
            _, back = jax.vjp(lambda w, h: layer(h, w), {name: w[number] for name, w in zip(NAMES, weights, strict=True)}, kept[number])
            by_w, by_h = back(by_h)
            own[number] = [by_w[name] for name in NAMES]
        gate, up, down = (jnp.stack([own[number][i] for number in range(layers)]) for i in range(3))
        down, gate, up = exchange(down, gate, up)
        gradients = [g.astype(jnp.float32) for g in (gate, up, down)]
        new = [adamw(w.astype(jnp.float32), m, v, g) for w, m, v, g in zip(weights, m, v, gradients, strict=True)]
        return tuple(one[which] for which in range(3) for one in new)

    return jax.shard_map(
        step,
        mesh=mesh,
        in_specs=(P(("rep", "dp"), None, None),) * 2 + (P(None, None, None),) * 9,
        out_specs=(P("rep", None, None),) * 9,
        check_vma=False,
    )
```

```python
import functools

import jax
import jax.numpy as jnp
from jax import lax
from jax.experimental import pallas as pl
from jax.experimental.pallas import tpu as pltpu
from jax.sharding import PartitionSpec as P

MESH = pl.DeviceIdType.MESH
DIMS = (4, 4, 8)
BLOCK = 512
TILE = 1024
FORWARD_TILE = 512
PERIOD = (("inputs",), ("back 0",), ("back 1",), ("down", "gate", "up"))
TICKS = len(PERIOD)
TN = (((0,), (0,)), ((), ()))
NT = (((1,), (1,)), ((), ()))
BF16, F32 = jnp.bfloat16, jnp.float32


def adamw(w, m, v, g):
    m = 0.9 * m + 0.1 * g
    v = 0.95 * v + 0.05 * g * g
    step = m * lax.rsqrt(v + 1e-8) + 0.1 * w
    return (w - 0.02 * step).astype(jnp.bfloat16), m, v


def ds(start, size, multiple=None):
    if isinstance(start, int):
        return pl.ds(start, size)
    return pl.ds(pl.multiple_of(start, multiple or size), size)


class Torus:
    def __init__(self):
        i = lax.axis_index("dp")
        nx, ny, nz = DIMS
        self.at = (lax.div(i, ny * nz), lax.rem(lax.div(i, nz), ny), lax.rem(i, nz))

    def shifted(self, axis, by):
        n = DIMS[axis]
        return lax.rem(self.at[axis] + (by % n), n)

    def device(self, axis, by):
        to = list(self.at)
        to[axis] = self.shifted(axis, by)
        return {"dp": (to[0] * DIMS[1] + to[1]) * DIMS[2] + to[2]}

    def barrier(self):
        sem = pltpu.get_barrier_semaphore()
        peers = [(axis, by) for axis in range(3) for by in range(1, DIMS[axis])]
        for axis, by in peers:
            pl.semaphore_signal(sem, inc=1, device_id=self.device(axis, by), device_id_type=MESH)
        return lambda: pl.semaphore_wait(sem, len(peers))


class Step:
    def __init__(self, start, finish):
        self.start, self.finish = start, finish


def rows_loop(rows, lanes, body):
    size = min(rows, max(16, 16 * (512 // lanes)))
    if rows == size:
        body(0, size)
        return

    def one(i, _):
        body(pl.multiple_of(i * size, size), size)
        return 0

    lax.fori_loop(0, rows // size, one, 0)


class Exchange:
    def __init__(self, torus, order, chained, chunk, rx, p32, pb, r32, rb, sems, sites):
        self.torus, self.order, self.chained = torus, order, chained
        self.chunk = chunk
        self.rx1, self.rx2, self.rx3 = rx
        self.p32, self.pb, self.r32, self.rb = p32, pb, r32, rb
        self.send_sems, self.recv_sems = sems
        self.sites = sites
        n1, n2, n3 = (DIMS[a] for a in order)
        self.rows1 = BLOCK // n1
        self.lanes2 = BLOCK // n2
        self.rows3 = self.rows1 // n3
        self.steps = self._steps()

    def _site(self):
        s = self.sites[0]
        self.sites[0] += 1
        return s

    def _copy(self, c, site, src, dst, axis, by):
        slot = c
        pltpu.make_async_remote_copy(
            src_ref=src,
            dst_ref=dst,
            send_sem=self.send_sems.at[slot, site],
            recv_sem=self.recv_sems.at[slot, site],
            device_id=self.torus.device(axis, by),
            device_id_type=MESH,
        ).start()

    def _wait(self, c, site, like, recv):
        sem = (self.recv_sems if recv else self.send_sems).at[c, site]
        pltpu.make_async_copy(like, like, sem).wait()

    def _chain(self, axis, rows, lanes, send_ref, own, rx, total):
        n = DIMS[axis]
        k = n // 2
        half = rows // 2
        ways = ((1, 0, 0), (-1, 1, half))
        steps = []
        for s in range(1, k + 1):
            sites = [self._site() for _ in ways]

            def start(c, s=s, sites=sites):
                for (way, w, h0), site in zip(ways, sites, strict=True):
                    t = self.torus.shifted(axis, way * (k + 1 - s))
                    dst = rx(c, w, s - 1)
                    if s == 1:
                        self._copy(c, site, send_ref(c, t, h0, half), dst.at[ds(h0, half), :], axis, way)
                    elif s == 2:
                        o0 = half - h0
                        self._copy(c, site, rx(c, w, 0).at[ds(h0, half), :], dst.at[ds(h0, half), :], axis, way)
                        self._copy(c, site, send_ref(c, t, o0, half), dst.at[ds(o0, half), :], axis, way)
                    else:
                        self._copy(c, site, rx(c, w, s - 2), dst, axis, way)

            def finish(c, s=s, sites=sites):
                for (way, w, h0), site in zip(ways, sites, strict=True):
                    got = rx(c, w, s - 1)
                    part = got.at[ds(h0, half), :] if s == 1 else got
                    self._wait(c, site, part, True)
                    if s < k:
                        t = self.torus.shifted(axis, way * (k - s))
                        first, count = (h0, half) if s == 1 else (0, rows)

                        def add(r0, size, got=got, t=t, first=first):
                            at = ds(first + r0, size, 16)
                            got[at, :] = (got[at, :].astype(F32) + own(c, t, first + r0, size)).astype(BF16)

                        rows_loop(count, lanes, add)
                if s == k:
                    me = self.torus.shifted(axis, 0)
                    for first in (0, half):

                        def add(r0, size, first=first):
                            at = ds(first + r0, size, 16)
                            value = own(c, me, first + r0, size)
                            for way, w, h0 in ways:
                                if k > 1 or h0 == first:
                                    value = value + rx(c, w, k - 1)[at, :].astype(F32)
                            total(c, first + r0, size, value)

                        rows_loop(half, lanes, add)
                for (way, w, h0), site in zip(ways, sites, strict=True):
                    got = rx(c, w, s - 1)
                    self._wait(c, site, got.at[ds(h0, half), :] if s == 1 else got, False)

            steps.append(Step(start, finish))
        return steps

    def _chain_gather(self, axis, rows, block):
        n = DIMS[axis]
        k = n // 2
        half = rows // 2
        ways = ((1, 0), (-1, half))
        steps = []
        for s in range(1, k + 1):
            sites = [self._site() for _ in ways]

            def start(c, s=s, sites=sites):
                for (way, h0), site in zip(ways, sites, strict=True):
                    t = self.torus.shifted(axis, -way * (s - 1))
                    ref = block(c, t, h0, half) if s == k else block(c, t, 0, rows)
                    self._copy(c, site, ref, ref, axis, way)

            def finish(c, s=s, sites=sites):
                for recv in (True, False):
                    for (way, h0), site in zip(ways, sites, strict=True):
                        t = self.torus.shifted(axis, -way * s)
                        self._wait(c, site, block(c, t, h0, half) if s == k else block(c, t, 0, rows), recv)

            steps.append(Step(start, finish))
        return steps

    def _direct(self, axis, rows, lanes, send_ref, own, rx, total):
        n = DIMS[axis]
        site = self._site()

        def start(c):
            for by in range(1, n):
                t = self.torus.shifted(axis, by)
                self._copy(c, site, send_ref(c, t), rx(c).at[by - 1], axis, by)

        def finish(c):
            self._wait(c, site, rx(c), True)

            def add(r0, size):
                value = own(c, r0, size)
                for i in range(n - 1):
                    value = value + rx(c)[i, ds(r0, size, 16), :].astype(F32)
                total(c, r0, size, value)

            rows_loop(rows, lanes, add)
            self._wait(c, site, rx(c), False)

        return [Step(start, finish)]

    def _direct_gather(self, axis, mine, like):
        n = DIMS[axis]
        site = self._site()

        def start(c):
            for by in range(1, n):
                self._copy(c, site, mine(c), mine(c), axis, by)

        def finish(c):
            self._wait(c, site, like(c), True)
            self._wait(c, site, like(c), False)

        return [Step(start, finish)]

    def _steps(self):
        a1, a2, a3 = self.order
        rows1, lanes2, rows3 = self.rows1, self.lanes2, self.rows3
        at = [self.torus.at[a] for a in self.order]
        chunk = self.chunk

        def block1(c, t, r0, n):
            return chunk(c).at[ds(t * rows1 + r0, n, 16), :]

        def own1(c, t, r0, n):
            return chunk(c)[ds(t * rows1 + r0, n, 16), :].astype(F32)

        def total1(c, r0, n, value):
            at_ = ds(r0, n, 16)
            self.p32[c % 2, at_, :] = value
            self.pb[c % 2, at_, :] = value.astype(BF16)

        steps = self._chain(a1, rows1, BLOCK, block1, own1, lambda c, w, s: self.rx1.at[c, w, s], total1)

        def own2(c, t, r0, n):
            return self.p32[c % 2, ds(r0, n, 16), ds(t * lanes2, lanes2)]

        def total2(c, r0, n, value):
            at_ = ds(r0, n, 16)
            self.r32[c % 2, at_, :] = value
            self.rb[c % 2, at_, :] = value.astype(BF16)

        if self.chained:
            steps += self._chain(
                a2,
                rows1,
                lanes2,
                lambda c, t, r0, n: self.pb.at[c % 2, ds(r0, n, 16), ds(t * lanes2, lanes2)],
                own2,
                lambda c, w, s: self.rx2.at[c, w, s],
                total2,
            )
        else:
            steps += self._direct(
                a2,
                rows1,
                lanes2,
                lambda c, t: self.pb.at[c % 2, :, ds(t * lanes2, lanes2)],
                lambda c, r0, n: own2(c, at[1], r0, n),
                lambda c: self.rx2.at[c],
                total2,
            )

        def final(c):
            return chunk(c).at[ds(at[0] * rows1 + at[2] * rows3, rows3, 16), ds(at[1] * lanes2, lanes2)]

        def total3(c, r0, n, value):
            final(c)[ds(r0, n, 16), :] = value.astype(BF16)

        steps += self._direct(
            a3,
            rows3,
            lanes2,
            lambda c, t: self.rb.at[c % 2, ds(t * rows3, rows3, 16), :],
            lambda c, r0, n: self.r32[c % 2, ds(at[2] * rows3 + r0, n, 16), :],
            lambda c: self.rx3.at[c],
            total3,
        )
        steps += self._direct_gather(a3, final, lambda c: self.rx3.at[c])

        def block2(c, t, r0, n):
            return chunk(c).at[ds(at[0] * rows1 + r0, n, 16), ds(t * lanes2, lanes2)]

        if self.chained:
            steps += self._chain_gather(a2, rows1, block2)
        else:
            steps += self._direct_gather(a2, lambda c: block2(c, at[1], 0, rows1), lambda c: self.rx2.at[c])
        steps += self._chain_gather(a1, rows1, block1)
        return steps

    @staticmethod
    def scratch(order, chained, chunks):
        n1, n2, n3 = (DIMS[a] for a in order)
        rows1, lanes2 = BLOCK // n1, BLOCK // n2
        rx2 = (chunks, 2, n2 // 2, rows1, lanes2) if chained else (chunks, n2 - 1, rows1, lanes2)
        return [
            pltpu.VMEM((chunks, 2, n1 // 2, rows1, BLOCK), BF16),
            pltpu.VMEM(rx2, BF16),
            pltpu.VMEM((chunks, n3 - 1, rows1 // n3, lanes2), BF16),
            pltpu.VMEM((2, rows1, BLOCK), F32),
            pltpu.VMEM((2, rows1, BLOCK), BF16),
            pltpu.VMEM((2, rows1, lanes2), F32),
            pltpu.VMEM((2, rows1, lanes2), BF16),
        ]

    @staticmethod
    def n_sites(order, chained):
        k1, k2 = DIMS[order[0]] // 2, DIMS[order[1]] // 2
        return 4 * k1 + (4 * k2 if chained else 2) + 2


COLOURS = (((0, 1, 2), True), ((1, 0, 2), True), ((2, 0, 1), False))


def dot(a, b, dims=(((1,), (0,)), ((), ()))):
    return lax.dot_general(a, b, dims, preferred_element_type=F32)


def inverse_rms(wide):
    return lax.rsqrt(jnp.mean(wide * wide, -1, keepdims=True) + 1e-6)


def normed(h):
    wide = h.astype(F32)
    return (wide * inverse_rms(wide)).astype(BF16)


def sigmoid(x):
    return 0.5 * jnp.tanh(0.5 * x) + 0.5


def tiles(rows, size, body):
    def one(i, _):
        body(pl.ds(pl.multiple_of(i * size, size), size))
        return 0

    lax.fori_loop(0, rows // size, one, 0)


class Compute:
    def __init__(self, weights, states, dh, a, by, da):
        self.w_gate, self.w_up, self.w_down = weights
        self.states = states
        self.dh = dh
        self.a = a
        self.by = by
        self.da = da

    def forward(self, number):
        rows, ff = self.a.shape[0], self.w_gate.shape[2]

        def body(at):
            h = self.states[number, at, :]
            a = normed(h)
            out = None
            for f in range(0, ff, BLOCK):
                columns = pl.ds(f, BLOCK)
                gate = dot(a, self.w_gate[number, :, columns])
                up = dot(a, self.w_up[number, :, columns])
                part = dot((gate * sigmoid(gate) * up).astype(BF16), self.w_down[number, columns, :])
                out = part if out is None else out + part
            h = h + out.astype(BF16)
            self.states[number + 1, at, :] = h
            self.a[at, :] = normed(h)

        tiles(rows, min(FORWARD_TILE, rows), body)

    def back(self, number, block, tile):
        columns = ds(block * BLOCK, BLOCK)
        size = min(TILE, self.a.shape[0] // 2)
        at = pl.ds(tile * size, size)
        a = self.a[at, :]
        gate = dot(a, self.w_gate[number, :, columns])
        up = dot(a, self.w_up[number, :, columns])
        by = dot(self.dh[at, :], self.w_down[number, columns, :], NT).astype(BF16).astype(F32)
        s = sigmoid(gate)
        silu = gate * s
        self.by[0, at, :] = (silu * up).astype(BF16)
        self.by[1, at, :] = (by * up * (s + silu * (1.0 - s))).astype(BF16)
        self.by[2, at, :] = (by * silu).astype(BF16)

    def gradient(self, which, into):
        if which == 0:
            into[...] = dot(self.by[0], self.dh[...], TN).astype(BF16)
        else:
            into[...] = dot(self.a[...], self.by[which], TN).astype(BF16)

    def inputs(self, number, block):
        columns = ds(block * BLOCK, BLOCK)
        rows = self.a.shape[0]

        def body(at):
            part = dot(self.by[1, at, :], self.w_gate[number, :, columns], NT)
            part = part + dot(self.by[2, at, :], self.w_up[number, :, columns], NT)
            self.da[at, :] = jnp.where(block == 0, 0.0, self.da[at, :]) + part

        tiles(rows, min(TILE, rows), body)

    def below(self, number):
        rows = self.a.shape[0]

        def body(at):
            wide = self.states[number, at, :].astype(F32)
            by = self.da[at, :].astype(BF16).astype(F32)
            scale = inverse_rms(wide)
            by = by * scale - wide * (scale * scale * scale * jnp.mean(by * wide, -1, keepdims=True))
            self.dh[at, :] = self.dh[at, :] + by.astype(BF16)
            self.a[at, :] = normed(self.states[number - 1, at, :])

        tiles(rows, min(256, rows), body)


def train_kernel(x, dy, w_gate, w_up, w_down, o_gate, o_up, o_down, *scratch):
    (s_gate, s_up, s_down, states, dh, a, by, da, g), scratch = scratch[:9], scratch[9:]
    scratch, (send_sems, recv_sems, out_sems, in_sems) = scratch[:-4], scratch[-4:]
    layers, _, ff = w_gate.shape
    blocks = ff // BLOCK
    chunks = layers * blocks
    assert layers == 2
    torus = Torus()
    loads = [pltpu.make_async_copy(x.at[0], states.at[0], in_sems.at[0])]
    for number in range(layers):
        for i, (src, dst) in enumerate(((w_gate, s_gate), (w_up, s_up), (w_down, s_down))):
            loads.append(pltpu.make_async_copy(src.at[number], dst.at[number], in_sems.at[1 + 3 * number + i]))
    loads.append(pltpu.make_async_copy(dy.at[0], dh, in_sems.at[1 + 3 * layers]))
    for copy in loads:
        copy.start()
    barrier = torus.barrier()
    compute = Compute((s_gate, s_up, s_down), states, dh, a, by, da)
    for copy in loads[:4]:
        copy.wait()
    compute.forward(0)
    for copy in loads[4:]:
        copy.wait()
    barrier()

    sites, exchanges = [0], []
    for k, (order, chained) in enumerate(COLOURS):
        rx, temporary = scratch[7 * k : 7 * k + 3], scratch[7 * k + 3 : 7 * k + 7]
        exchanges.append(Exchange(torus, order, chained, lambda c, k=k: g.at[c, k], rx, *temporary, (send_sems, recv_sems), sites))
    longest = max(len(e.steps) for e in exchanges)

    def save(c, k):
        number, j = layers - 1 - lax.div(c, blocks), lax.rem(c, blocks)
        place = o_down.at[number, ds(j * BLOCK, BLOCK), :] if k == 0 else (o_gate, o_up)[k - 1].at[number, :, ds(j * BLOCK, BLOCK)]
        return pltpu.make_async_copy(g.at[c, k], place, out_sems.at[c, k])

    def tick(s, period):
        for stage in range(s, longest + 1, TICKS):
            c = period - 1 - stage // TICKS

            @pl.when((c >= 0) & (c < chunks))
            def _(c=c, stage=stage):
                for k, e in enumerate(exchanges):
                    if 1 <= stage <= len(e.steps):
                        e.steps[stage - 1].finish(c)
                        if stage == len(e.steps):
                            save(c, k).start()
                for e in exchanges:
                    if stage < len(e.steps):
                        e.steps[stage].start(c)

    def work(name, period):
        number, block = layers - 1 - lax.div(period, blocks), lax.rem(period, blocks)
        if name == "inputs":
            before = period - 1

            @pl.when((before >= 0) & (before < chunks - blocks))
            def _():
                compute.inputs(layers - 1 - lax.div(before, blocks), lax.rem(before, blocks))

            @pl.when((period > 0) & (period < chunks) & (block == 0))
            def _():
                compute.below(number + 1)

            return

        @pl.when(period < chunks)
        def _():
            if name.startswith("back"):
                compute.back(number, block, int(name[5:]))
            else:
                which = ("down", "gate", "up").index(name)
                compute.gradient(which, g.at[period, which])

    def body(period, _):
        for s in range(TICKS):
            tick(s, period)
            for name in PERIOD[s]:
                work(name, period)
        return 0

    lax.fori_loop(0, chunks + 1 + longest // TICKS, body, 0)
    for c in range(chunks):
        for k in range(3):
            save(c, k).wait()


def gradients(x, dy, gate, up, down):
    layers, d, ff = gate.shape
    tokens = x.shape[1]
    chunks = layers * ff // BLOCK
    scratch = [
        *(pltpu.VMEM(w.shape, BF16) for w in (gate, up, down)),
        pltpu.VMEM((layers, tokens, d), BF16),
        pltpu.VMEM((tokens, d), BF16),
        pltpu.VMEM((tokens, d), BF16),
        pltpu.VMEM((3, tokens, BLOCK), BF16),
        pltpu.VMEM((tokens, d), F32),
        pltpu.VMEM((chunks, 3, BLOCK, BLOCK), BF16),
    ]
    n_sites = 0
    for order, chained in COLOURS:
        scratch += Exchange.scratch(order, chained, chunks)
        n_sites += Exchange.n_sites(order, chained)
    scratch += [pltpu.SemaphoreType.DMA((chunks, n_sites))] * 2
    scratch += [pltpu.SemaphoreType.DMA((chunks, 3)), pltpu.SemaphoreType.DMA((2 + 3 * layers,))]
    return pl.pallas_call(
        train_kernel,
        out_shape=[jax.ShapeDtypeStruct(w.shape, BF16) for w in (gate, up, down)],
        in_specs=[pl.BlockSpec(memory_space=pl.ANY)] * 5,
        out_specs=[pl.BlockSpec(memory_space=pl.ANY)] * 3,
        scratch_shapes=scratch,
        compiler_params=pltpu.CompilerParams(collective_id=0, has_side_effects=True, vmem_limit_bytes=63 << 20),
        name="gradients",
    )(x, dy, gate, up, down)


def solution(mesh):
    def step(x, dy, *arrays):
        weights, m, v = (arrays[i : i + 3] for i in (0, 3, 6))
        summed = [g.astype(F32) for g in gradients(x, dy, *weights)]
        new = [adamw(w.astype(F32), m, v, g) for w, m, v, g in zip(weights, m, v, summed, strict=True)]
        return tuple(one[which] for which in range(3) for one in new)

    return jax.shard_map(
        step,
        mesh=mesh,
        in_specs=(P(("rep", "dp"), None, None),) * 2 + (P(None, None, None),) * 9,
        out_specs=(P("rep", None, None),) * 9,
        check_vma=False,
    )
```

```python
import functools

import jax
import jax.numpy as jnp
from jax import lax
from jax.experimental import pallas as pl
from jax.experimental.pallas import tpu as pltpu
from jax.sharding import PartitionSpec as P

MESH = pl.DeviceIdType.MESH
DIMS = (4, 4, 8)
BLOCK = 512
TILE = 512
PIECE = 128
STRIP = 32
SLOTS = 3
OUTPUTS = 4
PERIOD = (
    "below",
    (2, 8, 3), (0, 7, 3),
    "back 0",
    (2, 5, 2), (1, 1, 1), (0, 9, 4), (1, 7, 3), (2, 2, 1),
    "back 1",
    (0, 2, 1), (1, 9, 4), (2, 11, 4), (0, 5, 2),
    "back 2",
    (0, 8, 3), (2, 6, 2), (1, 5, 2), (1, 2, 1), (2, 9, 3),
    "back 3",
    (2, 3, 1), (0, 3, 1), (1, 8, 3),
    "up",
    (2, 7, 2), (0, 10, 4), (1, 10, 4), (2, 12, 4), (2, 0, 0),
    "down",
    (0, 0, 0), (2, 10, 3), (0, 6, 2), (0, 4, 1), (1, 3, 1), (2, 4, 1),
    "gate",
    (1, 0, 0), (2, 1, 0),
    "inputs 0",
    (1, 6, 2),
    "inputs 1",
    (0, 1, 0), (1, 4, 1),
)
VMEM_LIMIT = UPDATE_LIMIT = 29_200_000
TN = (((0,), (0,)), ((), ()))
NT = (((1,), (1,)), ((), ()))
BF16, F32 = jnp.bfloat16, jnp.float32


def ds(start, size, multiple=None):
    if isinstance(start, int):
        return pl.ds(start, size)
    return pl.ds(pl.multiple_of(start, multiple or size), size)


class Torus:
    def __init__(self):
        i = lax.axis_index("dp")
        nx, ny, nz = DIMS
        self.at = (lax.div(i, ny * nz), lax.rem(lax.div(i, nz), ny), lax.rem(i, nz))
        self._places, self._devices = {}, {}
        for axis, n in enumerate(DIMS):
            for by in range(n):
                self._places[axis, by] = place = lax.rem(self.at[axis] + by, n) if by else self.at[axis]
                to = list(self.at)
                to[axis] = place
                self._devices[axis, by] = (to[0] * ny + to[1]) * nz + to[2]

    def shifted(self, axis, by):
        return self._places[axis, by % DIMS[axis]]

    def device(self, axis, by):
        return {"dp": self._devices[axis, by % DIMS[axis]]}

    def barrier(self):
        sem = pltpu.get_barrier_semaphore()
        peers = [(axis, by) for axis in range(3) for by in range(1, DIMS[axis])]
        for axis, by in peers:
            pl.semaphore_signal(sem, inc=1, device_id=self.device(axis, by), device_id_type=MESH)
        return lambda: pl.semaphore_wait(sem, len(peers))


class Step:
    def __init__(self, start, finish):
        self.start, self.finish = start, finish


def rows_loop(rows, lanes, body):
    size = min(rows, 32 * 1024 // lanes)
    for r0 in range(0, rows, size):
        body(r0, size)


class Exchange:
    def __init__(self, torus, order, chained, chunk, rx, p32, pb, r32, rb, sems, sites):
        self.torus, self.order, self.chained = torus, order, chained
        self.chunk = chunk
        self.rx1, self.rx2, self.rx3 = rx
        self.p32, self.pb, self.r32, self.rb = p32, pb, r32, rb
        self.send_sems, self.recv_sems = sems
        self.sites = sites
        n1, n2, n3 = (DIMS[a] for a in order)
        self.rows1 = BLOCK // n1
        self.lanes2 = BLOCK // n2
        self.rows3 = self.rows1 // n3
        self.steps = self._steps()

    def _site(self):
        s = self.sites[0]
        self.sites[0] += 1
        return s

    def _copy(self, c, site, src, dst, axis, by):
        pltpu.make_async_remote_copy(
            src_ref=src,
            dst_ref=dst,
            send_sem=self.send_sems.at[lax.rem(c, SLOTS), site],
            recv_sem=self.recv_sems.at[lax.rem(c, SLOTS), site],
            device_id=self.torus.device(axis, by),
            device_id_type=MESH,
        ).start()

    def _arrived(self, c, site, like):
        pltpu.make_async_copy(like, like, self.recv_sems.at[lax.rem(c, SLOTS), site]).wait()

    def _left(self, c, site, like):
        pltpu.make_async_copy(like, like, self.send_sems.at[lax.rem(c, SLOTS), site]).wait()

    def _chain(self, axis, rows, lanes, send_ref, own, rx, total):
        n = DIMS[axis]
        k = n // 2
        half = rows // 2
        ways = ((1, 0, 0), (-1, 1, half))
        steps = []
        for s in range(1, k + 1):
            site = self._site()

            def start(c, s=s, site=site):
                for way, w, h0 in ways:
                    t = self.torus.shifted(axis, way * (k + 1 - s))
                    dst = rx(c, s - 1).at[w]
                    if s == 1:
                        self._copy(c, site, send_ref(c, t, h0, half), dst.at[ds(h0, half), :], axis, way)
                    elif s == 2:
                        o0 = half - h0
                        self._copy(c, site, rx(c, 0).at[w, ds(h0, half), :], dst.at[ds(h0, half), :], axis, way)
                        self._copy(c, site, send_ref(c, t, o0, half), dst.at[ds(o0, half), :], axis, way)
                    else:
                        self._copy(c, site, rx(c, s - 2).at[w], dst, axis, way)

            def finish(c, s=s, site=site):
                got = rx(c, s - 1)
                like = got.at[0] if s == 1 else got
                self._arrived(c, site, like)
                if s < k:
                    for way, w, h0 in ways:
                        t = self.torus.shifted(axis, way * (k - s))
                        first, count = (h0, half) if s == 1 else (0, rows)

                        def add(r0, size, w=w, t=t, first=first):
                            at = pl.ds(first + r0, size)
                            got[w, at, :] = (got[w, at, :].astype(F32) + own(c, t, first + r0, size)).astype(BF16)

                        rows_loop(count, lanes, add)
                else:
                    me = self.torus.shifted(axis, 0)
                    for first in (0, half):

                        def add(r0, size, first=first):
                            at = pl.ds(first + r0, size)
                            value = own(c, me, first + r0, size)
                            for way, w, h0 in ways:
                                if k > 1 or h0 == first:
                                    value = value + got[w, at, :].astype(F32)
                            total(c, first + r0, size, value)

                        rows_loop(half, lanes, add)
                self._left(c, site, like)

            steps.append(Step(start, finish))
        return steps

    def _chain_gather(self, axis, rows, block, like):
        n = DIMS[axis]
        k = n // 2
        half = rows // 2
        ways = ((1, 0), (-1, half))
        steps = []
        for s in range(1, k + 1):
            site = self._site()

            def start(c, s=s, site=site):
                for way, h0 in ways:
                    t = self.torus.shifted(axis, -way * (s - 1))
                    ref = block(c, t, h0, half) if s == k else block(c, t, 0, rows)
                    self._copy(c, site, ref, ref, axis, way)

            def finish(c, s=s, site=site):
                both = like(c, 1 if s == k else 2)
                self._arrived(c, site, both)
                self._left(c, site, both)

            steps.append(Step(start, finish))
        return steps

    def _direct(self, axis, rows, lanes, send_ref, own, rx, total):
        n = DIMS[axis]
        site = self._site()

        def start(c):
            for by in range(1, n):
                t = self.torus.shifted(axis, by)
                self._copy(c, site, send_ref(c, t), rx(c).at[by - 1], axis, by)

        def finish(c):
            self._arrived(c, site, rx(c))

            def add(r0, size):
                value = own(c, r0, size)
                for i in range(n - 1):
                    value = value + rx(c)[i, pl.ds(r0, size), :].astype(F32)
                total(c, r0, size, value)

            rows_loop(rows, lanes, add)
            self._left(c, site, rx(c))

        return [Step(start, finish)]

    def _direct_gather(self, axis, mine, like):
        n = DIMS[axis]
        site = self._site()

        def start(c):
            for by in range(1, n):
                self._copy(c, site, mine(c), mine(c), axis, by)

        def finish(c):
            self._arrived(c, site, like(c))
            self._left(c, site, like(c))

        return [Step(start, finish)]

    def _steps(self):
        a1, a2, a3 = self.order
        rows1, lanes2, rows3 = self.rows1, self.lanes2, self.rows3
        at = [self.torus.at[a] for a in self.order]
        chunk = self.chunk

        def block1(c, t, r0, n):
            return chunk(c).at[ds(t * rows1 + r0, n, 16), :]

        def own1(c, t, r0, n):
            return chunk(c)[ds(t * rows1 + r0, n, 16), :].astype(F32)

        def total1(c, r0, n, value):
            at_ = ds(r0, n, 16)
            self.p32[at_, :] = value
            self.pb[at_, :] = value.astype(BF16)

        steps = self._chain(a1, rows1, BLOCK, block1, own1, lambda c, s: self.rx1.at[lax.rem(c, SLOTS), s], total1)

        def own2(c, t, r0, n):
            return self.p32[ds(r0, n, 16), ds(t * lanes2, lanes2)]

        def total2(c, r0, n, value):
            at_ = ds(r0, n, 16)
            self.r32[at_, :] = value
            self.rb[at_, :] = value.astype(BF16)

        if self.chained:
            steps += self._chain(
                a2,
                rows1,
                lanes2,
                lambda c, t, r0, n: self.pb.at[ds(r0, n, 16), ds(t * lanes2, lanes2)],
                own2,
                lambda c, s: self.rx2.at[lax.rem(c, SLOTS), s],
                total2,
            )
        else:
            steps += self._direct(
                a2,
                rows1,
                lanes2,
                lambda c, t: self.pb.at[:, ds(t * lanes2, lanes2)],
                lambda c, r0, n: own2(c, at[1], r0, n),
                lambda c: self.rx2.at[lax.rem(c, SLOTS)],
                total2,
            )

        def final(c):
            return chunk(c).at[ds(at[0] * rows1 + at[2] * rows3, rows3, 16), ds(at[1] * lanes2, lanes2)]

        def total3(c, r0, n, value):
            final(c)[ds(r0, n, 16), :] = value.astype(BF16)

        steps += self._direct(
            a3,
            rows3,
            lanes2,
            lambda c, t: self.rb.at[ds(t * rows3, rows3, 16), :],
            lambda c, r0, n: self.r32[ds(at[2] * rows3 + r0, n, 16), :],
            lambda c: self.rx3.at[lax.rem(c, SLOTS)],
            total3,
        )
        steps += self._direct_gather(a3, final, lambda c: self.rx3.at[lax.rem(c, SLOTS)])

        def block2(c, t, r0, n):
            return chunk(c).at[ds(at[0] * rows1 + r0, n, 16), ds(t * lanes2, lanes2)]

        if self.chained:
            steps += self._chain_gather(a2, rows1, block2, lambda c, n: chunk(c).at[pl.ds(0, rows1), pl.ds(0, n * lanes2)])
        else:
            steps += self._direct_gather(a2, lambda c: block2(c, at[1], 0, rows1), lambda c: self.rx2.at[lax.rem(c, SLOTS)])
        steps += self._chain_gather(a1, rows1, block1, lambda c, n: chunk(c).at[pl.ds(0, n * rows1), :])
        return steps

    @staticmethod
    def scratch(order, chained, chunks):
        n1, n2, n3 = (DIMS[a] for a in order)
        rows1, lanes2 = BLOCK // n1, BLOCK // n2
        rx2 = (chunks, n2 // 2, 2, rows1, lanes2) if chained else (chunks, n2 - 1, rows1, lanes2)
        return [
            pltpu.VMEM((chunks, n1 // 2, 2, rows1, BLOCK), BF16),
            pltpu.VMEM(rx2, BF16),
            pltpu.VMEM((chunks, n3 - 1, rows1 // n3, lanes2), BF16),
            pltpu.VMEM((rows1, BLOCK), F32),
            pltpu.VMEM((rows1, BLOCK), BF16),
            pltpu.VMEM((rows1, lanes2), F32),
            pltpu.VMEM((rows1, lanes2), BF16),
        ]

    @staticmethod
    def n_sites(order, chained):
        k1, k2 = DIMS[order[0]] // 2, DIMS[order[1]] // 2
        return 2 * k1 + (2 * k2 if chained else 2) + 2


DOWN, GATE, UP = range(3)
COLOURS = (((0, 1, 2), True), ((1, 0, 2), True), ((2, 0, 1), False))


def dot(a, b, dims=(((1,), (0,)), ((), ()))):
    return lax.dot_general(a, b, dims, preferred_element_type=F32)


def inverse_rms(wide):
    return lax.rsqrt(jnp.mean(wide * wide, -1, keepdims=True) + 1e-6)


def normed(h):
    wide = h.astype(F32)
    return (wide * inverse_rms(wide)).astype(BF16)


def sigmoid(x):
    return 0.5 * jnp.tanh(0.5 * x) + 0.5


def tiles(rows, size, body):
    def one(i, _):
        body(pl.ds(pl.multiple_of(i * size, size), size))
        return 0

    lax.fori_loop(0, rows // size, one, 0)


class Compute:
    def __init__(self, weights, states, dh, a, by, da):
        self.weights = weights
        self.states = states
        self.dh = dh
        self.a = a
        self.by = by
        self.da = da

    def forward(self, number):
        rows, blocks = self.a.shape[0], self.weights.shape[2]

        def body(at):
            h = self.states[number, at, :]
            a = normed(h)
            out = None
            for block in range(blocks):
                gate = dot(a, self.weights[GATE, number, block])
                up = dot(a, self.weights[UP, number, block])
                part = dot((gate * sigmoid(gate) * up).astype(BF16), self.weights[DOWN, number, block])
                out = part if out is None else out + part
            h = h + out.astype(BF16)
            self.states[number + 1, at, :] = h
            self.a[at, :] = normed(h)

        tiles(rows, min(TILE, rows), body)

    def back(self, number, block, tile):
        size = self.a.shape[0] // 4
        at = pl.ds(tile * size, size)
        a = self.a[at, :]
        gate = dot(a, self.weights[GATE, number, block])
        up = dot(a, self.weights[UP, number, block])
        by = dot(self.dh[at, :], self.weights[DOWN, number, block], NT).astype(BF16).astype(F32)
        s = sigmoid(gate)
        silu = gate * s
        self.by[DOWN, at, :] = (silu * up).astype(BF16)
        self.by[GATE, at, :] = (by * up * (s + silu * (1.0 - s))).astype(BF16)
        self.by[UP, at, :] = (by * silu).astype(BF16)

    def gradient(self, which, into):
        if which == DOWN:
            into[...] = dot(self.by[DOWN], self.dh[...], TN).astype(BF16)
        else:
            into[...] = dot(self.a[...], self.by[which], TN).astype(BF16)

    def inputs(self, number, block, tile):
        size = self.a.shape[0] // 2
        at = pl.ds(tile * size, size)
        part = dot(self.by[GATE, at, :], self.weights[GATE, number, block], NT)
        part = part + dot(self.by[UP, at, :], self.weights[UP, number, block], NT)
        self.da[at, :] = jnp.where(block == 0, 0.0, self.da[at, :]) + part

    def below(self, number):
        rows = self.a.shape[0]

        def body(at):
            wide = self.states[number, at, :].astype(F32)
            by = self.da[at, :].astype(BF16).astype(F32)
            scale = inverse_rms(wide)
            by = by * scale - wide * (scale * scale * scale * jnp.mean(by * wide, -1, keepdims=True))
            self.dh[at, :] = self.dh[at, :] + by.astype(BF16)
            self.a[at, :] = normed(self.states[number - 1, at, :])

        tiles(rows, min(256, rows), body)


def block_at(arrays, which, number, j, r0=0, n=BLOCK):
    if which == DOWN:
        return arrays[2].at[number, ds(j * BLOCK + r0, n), :]
    return arrays[which - 1].at[number, ds(r0, n), ds(j * BLOCK, BLOCK)]


def train_kernel(x, dy, *refs):
    weights, moments, (g, w, kept), refs = refs[:3], (refs[3:6], refs[6:9]), refs[9:12], refs[12:]
    (states, dh, a, by, da), scratch = refs[:5], refs[5:]
    scratch, (send_sems, recv_sems, in_sems) = scratch[:-3], scratch[-3:]
    _, layers, blocks, _, _ = w.shape
    chunks = layers * blocks
    assert layers == 2
    torus = Torus()
    wait_barrier = torus.barrier()
    early = [(x.at[0], states.at[0])]
    early += [(block_at(weights, which, 0, j), w.at[which, 0, j]) for j in range(blocks) for which in (GATE, UP, DOWN)]
    late = [(block_at(weights, which, 1, j), w.at[which, 1, j]) for j in range(blocks) for which in (GATE, UP, DOWN)]
    late.append((dy.at[0], dh))
    idle = [
        (block_at(moments[k], which, layers - 1, j), kept.at[k, which, j])
        for k in range(2)
        for which in range(3)
        for j in range(blocks)
    ]

    def copies(pairs, group):
        return [pltpu.make_async_copy(src, dst, in_sems.at[group, i]) for i, (src, dst) in enumerate(pairs)]

    early, late, idle = (copies(pairs, group) for group, pairs in enumerate((early, late, idle)))
    for copy in (*early, *late):
        copy.start()
    compute = Compute(w, states, dh, a, by, da)
    for copy in early:
        copy.wait()
    compute.forward(0)
    for copy in late:
        copy.wait()
    for copy in idle:
        copy.start()
    wait_barrier()

    sites, exchanges = [0], []
    for k, (order, chained) in enumerate(COLOURS):
        rx, temporary = scratch[7 * k : 7 * k + 3], scratch[7 * k + 3 : 7 * k + 7]
        exchanges.append(Exchange(torus, order, chained, lambda c, k=k: g.at[c, k], rx, *temporary, (send_sems, recv_sems), sites))

    def stage(c, k, s):
        steps = exchanges[k].steps
        if s:
            steps[s - 1].finish(c)
        if s < len(steps):
            steps[s].start(c)

    def work(name, c):
        number, block = layers - 1 - lax.div(c, blocks), lax.rem(c, blocks)
        if name == "below":

            @pl.when((c > 0) & (c < chunks) & (block == 0))
            def _():
                compute.below(number + 1)

            return
        what, _, tile = name.partition(" ")

        @pl.when(c < (chunks - blocks if what == "inputs" else chunks))
        def _():
            if what == "back":
                compute.back(number, block, int(tile))
            elif what == "inputs":
                compute.inputs(number, block, int(tile))
            else:
                which = ("down", "gate", "up").index(what)
                compute.gradient(which, g.at[c, which])

    lags = [item[2] for item in PERIOD if not isinstance(item, str)]

    def body(period, _):
        i = 0
        while i < len(PERIOD):
            if isinstance(PERIOD[i], str):
                work(PERIOD[i], period)
                i += 1
                continue
            j = i
            while j < len(PERIOD) and not isinstance(PERIOD[j], str) and PERIOD[j][2] == PERIOD[i][2]:
                j += 1
            c = period - PERIOD[i][2]

            @pl.when((c >= 0) & (c < chunks))
            def _(c=c, group=PERIOD[i:j]):
                for k, s, _ in group:
                    stage(c, k, s)

            i = j
        return 0

    lax.fori_loop(0, chunks + max(lags), body, 0)
    for copy in idle:
        copy.wait()


def gradients(x, dy, weights, moments):
    gate, up, down = weights
    layers, d, ff = gate.shape
    tokens = x.shape[1]
    chunks = layers * ff // BLOCK
    scratch = [
        pltpu.VMEM((layers, tokens, d), BF16),
        pltpu.VMEM((tokens, d), BF16),
        pltpu.VMEM((tokens, d), BF16),
        pltpu.VMEM((3, tokens, BLOCK), BF16),
        pltpu.VMEM((tokens, d), F32),
    ]
    n_sites = 0
    for order, chained in COLOURS:
        scratch += Exchange.scratch(order, chained, SLOTS)
        n_sites += Exchange.n_sites(order, chained)
    scratch += [pltpu.SemaphoreType.DMA((SLOTS, n_sites))] * 2 + [pltpu.SemaphoreType.DMA((3, 6 * ff // BLOCK))]
    out = [
        pltpu.VMEM((chunks, 3, BLOCK, BLOCK), BF16),
        pltpu.VMEM((3, layers, ff // BLOCK, BLOCK, BLOCK), BF16),
        pltpu.VMEM((2, 3, ff // BLOCK, BLOCK, BLOCK), F32),
    ]
    return pl.pallas_call(
        train_kernel,
        out_shape=out,
        in_specs=[pl.BlockSpec(memory_space=pltpu.HBM)] * 11,
        out_specs=[pl.BlockSpec(memory_space=pltpu.VMEM)] * len(out),
        scratch_shapes=scratch,
        compiler_params=pltpu.CompilerParams(collective_id=0, has_side_effects=True, vmem_limit_bytes=VMEM_LIMIT),
        name="gradients",
    )(x, dy, *weights, *moments)


def adamw(w, m, v, g):
    m = 0.9 * m + 0.1 * g
    v = 0.95 * v + 0.05 * g * g
    step = m * lax.rsqrt(v + 1e-8) + 0.1 * w
    return (w - 0.02 * step).astype(BF16), m, v


def adamw_kernel(g, w, kept, *refs):
    moments, new, refs = (refs[:3], refs[3:6]), (refs[6:9], refs[9:12], refs[12:15]), refs[15:]
    first, *staged, in_sems, out_sems = refs
    _, layers, blocks, _, _ = w.shape
    parts = BLOCK // PIECE

    def load(which, j):
        return [
            pltpu.make_async_copy(block_at(moments[k], which, 0, j), first.at[k, which, j], in_sems.at[k, which, j])
            for k in range(2)
        ]

    def save(number, slot, which, j, r0):
        return [
            pltpu.make_async_copy(staged[k].at[number, slot], block_at(new[k], which, number, j, r0, PIECE), out_sems.at[number, slot, k])
            for k in range(3)
        ]

    for which in range(3):
        for j in range(blocks):
            for copy in load(which, j):
                copy.start()

    for which in range(3):

        def one(i, _, which=which):
            j, r = lax.div(i, parts), lax.rem(i, parts)
            slot = lax.rem(i, OUTPUTS)

            @pl.when(r == 0)
            def _():
                for copy in load(which, j):
                    copy.wait()

            for number in reversed(range(layers)):

                @pl.when(which * blocks * parts + i >= OUTPUTS)
                def _(number=number):
                    for copy in save(number, slot, which, j, r * PIECE):
                        copy.wait()

                moment = kept if number else first
                for r0 in range(0, PIECE, STRIP):
                    rows = ds(r * PIECE + r0, STRIP)
                    grad = g[(layers - 1 - number) * blocks + j, which, rows, :].astype(F32)
                    now = adamw(w[which, number, j, rows, :].astype(F32), moment[0, which, j, rows, :], moment[1, which, j, rows, :], grad)
                    for k in range(3):
                        staged[k][number, slot, pl.ds(r0, STRIP), :] = now[k]
                for copy in save(number, slot, which, j, r * PIECE):
                    copy.start()
            return 0

        lax.fori_loop(0, blocks * parts, one, 0)
    for slot in range(OUTPUTS):
        for number in range(layers):
            for copy in save(number, slot, DOWN, 0, 0):
                copy.wait()


def update(g, w, kept, weights, moments):
    _, layers, blocks, _, _ = w.shape
    vmem, hbm = pl.BlockSpec(memory_space=pltpu.VMEM), pl.BlockSpec(memory_space=pltpu.HBM)
    return pl.pallas_call(
        adamw_kernel,
        out_shape=[jax.ShapeDtypeStruct(a.shape, BF16) for a in weights] + [jax.ShapeDtypeStruct(a.shape, F32) for a in moments],
        in_specs=[vmem] * 3 + [hbm] * 6,
        out_specs=[hbm] * 9,
        scratch_shapes=[
            pltpu.VMEM((2, 3, blocks, BLOCK, BLOCK), F32),
            *(pltpu.VMEM((layers, OUTPUTS, PIECE, BLOCK), dtype) for dtype in (BF16, F32, F32)),
            pltpu.SemaphoreType.DMA((2, 3, blocks)),
            pltpu.SemaphoreType.DMA((layers, OUTPUTS, 3)),
        ],
        compiler_params=pltpu.CompilerParams(vmem_limit_bytes=UPDATE_LIMIT),
        name="update",
    )(g, w, kept, *moments)


def solution(mesh):
    def step(x, dy, *arrays):
        weights, moments = arrays[:3], arrays[3:]
        there = gradients(x, dy, weights, moments)
        there = [pltpu.with_memory_space_constraint(a, pltpu.VMEM) for a in there]
        moments = [pltpu.with_memory_space_constraint(a, pltpu.HBM) for a in moments]
        return tuple(update(*there, weights, moments))

    return jax.shard_map(
        step,
        mesh=mesh,
        in_specs=(P(("rep", "dp"), None, None),) * 2 + (P(None, None, None),) * 9,
        out_specs=(P("rep", None, None),) * 9,
        check_vma=False,
    )
```

```python
import functools

import jax
import jax.numpy as jnp
from jax import lax
from jax.experimental import pallas as pl
from jax.experimental.pallas import tpu as pltpu
from jax.sharding import PartitionSpec as P

MESH = pl.DeviceIdType.MESH
DIMS = (4, 4, 8)
BLOCK = 512
TILE = 512
PIECE = 128
STRIP = 32
SLOTS = 3
OUTPUTS = 4
PERIOD = (
    "below",
    (1, 3, 2), (0, 1, 1), (1, 7, 4), (1, 9, 5), (0, 8, 4),
    "back 0",
    (0, 4, 2),
    "back 1",
    (2, 2, 1), (0, 6, 3), (2, 11, 5), (2, 5, 2),
    "back 2",
    (1, 4, 2), (2, 8, 3),
    "back 3",
    (0, 2, 1), (0, 10, 5), (1, 1, 1),
    "up",
    (2, 0, 0), (2, 3, 1), (2, 6, 2), (1, 8, 4), (1, 6, 3), (0, 7, 3),
    "down",
    (0, 0, 0), (0, 5, 2), (0, 3, 1), (2, 10, 4),
    "gate",
    (1, 2, 1), (2, 12, 5), (0, 9, 4), (1, 5, 2),
    "inputs 0",
    (1, 0, 0), (2, 4, 1), (2, 1, 0), (2, 9, 3),
    "inputs 1",
    (2, 7, 2), (1, 10, 5),
)
VMEM_LIMIT = UPDATE_LIMIT = 29_200_000
TN = (((0,), (0,)), ((), ()))
NT = (((1,), (1,)), ((), ()))
BF16, F32 = jnp.bfloat16, jnp.float32


def ds(start, size, multiple=None):
    if isinstance(start, int):
        return pl.ds(start, size)
    return pl.ds(pl.multiple_of(start, multiple or size), size)


class Torus:
    def __init__(self):
        i = lax.axis_index("dp")
        nx, ny, nz = DIMS
        self.at = (lax.div(i, ny * nz), lax.rem(lax.div(i, nz), ny), lax.rem(i, nz))
        self._places, self._devices = {}, {}
        for axis, n in enumerate(DIMS):
            for by in range(n):
                self._places[axis, by] = place = lax.rem(self.at[axis] + by, n) if by else self.at[axis]
                to = list(self.at)
                to[axis] = place
                self._devices[axis, by] = (to[0] * ny + to[1]) * nz + to[2]

    def shifted(self, axis, by):
        return self._places[axis, by % DIMS[axis]]

    def device(self, axis, by):
        return {"dp": self._devices[axis, by % DIMS[axis]]}

    def barrier(self):
        sem = pltpu.get_barrier_semaphore()
        peers = [(axis, by) for axis in range(3) for by in range(1, DIMS[axis])]
        for axis, by in peers:
            pl.semaphore_signal(sem, inc=1, device_id=self.device(axis, by), device_id_type=MESH)
        return lambda: pl.semaphore_wait(sem, len(peers))


class Step:
    def __init__(self, start, finish):
        self.start, self.finish = start, finish


def rows_loop(rows, lanes, body):
    size = min(rows, 32 * 1024 // lanes)
    for r0 in range(0, rows, size):
        body(r0, size)


class Exchange:
    def __init__(self, torus, order, chained, chunk, rx, p32, pb, r32, rb, sems, sites):
        self.torus, self.order, self.chained = torus, order, chained
        self.chunk = chunk
        self.rx1, self.rx2, self.rx3 = rx
        self.p32, self.pb, self.r32, self.rb = p32, pb, r32, rb
        self.send_sems, self.recv_sems = sems
        self.sites = sites
        n1, n2, n3 = (DIMS[a] for a in order)
        self.rows1 = BLOCK // n1
        self.lanes2 = BLOCK // n2
        self.rows3 = self.rows1 // n3
        self.steps = self._steps()

    def _site(self):
        s = self.sites[0]
        self.sites[0] += 1
        return s

    def _copy(self, c, site, src, dst, axis, by):
        pltpu.make_async_remote_copy(
            src_ref=src,
            dst_ref=dst,
            send_sem=self.send_sems.at[lax.rem(c, SLOTS), site],
            recv_sem=self.recv_sems.at[lax.rem(c, SLOTS), site],
            device_id=self.torus.device(axis, by),
            device_id_type=MESH,
        ).start()

    def _arrived(self, c, site, like):
        pltpu.make_async_copy(like, like, self.recv_sems.at[lax.rem(c, SLOTS), site]).wait()

    def _left(self, c, site, like):
        pltpu.make_async_copy(like, like, self.send_sems.at[lax.rem(c, SLOTS), site]).wait()

    def _chain(self, axis, rows, lanes, send_ref, own, rx, total):
        n = DIMS[axis]
        k = n // 2
        half = rows // 2
        ways = ((1, 0, 0), (-1, 1, half))
        steps = []
        for s in range(1, k + 1):
            site = self._site()

            def start(c, s=s, site=site):
                for way, w, h0 in ways:
                    t = self.torus.shifted(axis, way * (k + 1 - s))
                    dst = rx(c, s - 1).at[w]
                    if s == 1:
                        self._copy(c, site, send_ref(c, t, h0, half), dst.at[ds(h0, half), :], axis, way)
                    elif s == 2:
                        o0 = half - h0
                        self._copy(c, site, rx(c, 0).at[w, ds(h0, half), :], dst.at[ds(h0, half), :], axis, way)
                        self._copy(c, site, send_ref(c, t, o0, half), dst.at[ds(o0, half), :], axis, way)
                    else:
                        self._copy(c, site, rx(c, s - 2).at[w], dst, axis, way)

            def finish(c, s=s, site=site):
                got = rx(c, s - 1)
                like = got.at[0] if s == 1 else got
                self._arrived(c, site, like)
                if s < k:
                    for way, w, h0 in ways:
                        t = self.torus.shifted(axis, way * (k - s))
                        first, count = (h0, half) if s == 1 else (0, rows)

                        def add(r0, size, w=w, t=t, first=first):
                            at = pl.ds(first + r0, size)
                            got[w, at, :] = (got[w, at, :].astype(F32) + own(c, t, first + r0, size)).astype(BF16)

                        rows_loop(count, lanes, add)
                else:
                    me = self.torus.shifted(axis, 0)
                    for first in (0, half):

                        def add(r0, size, first=first):
                            at = pl.ds(first + r0, size)
                            value = own(c, me, first + r0, size)
                            for way, w, h0 in ways:
                                if k > 1 or h0 == first:
                                    value = value + got[w, at, :].astype(F32)
                            total(c, first + r0, size, value)

                        rows_loop(half, lanes, add)
                self._left(c, site, like)

            steps.append(Step(start, finish))
        return steps

    def _chain_gather(self, axis, rows, block, like):
        n = DIMS[axis]
        k = n // 2
        half = rows // 2
        ways = ((1, 0), (-1, half))
        steps = []
        for s in range(1, k + 1):
            site = self._site()

            def start(c, s=s, site=site):
                for way, h0 in ways:
                    t = self.torus.shifted(axis, -way * (s - 1))
                    ref = block(c, t, h0, half) if s == k else block(c, t, 0, rows)
                    self._copy(c, site, ref, ref, axis, way)

            def finish(c, s=s, site=site):
                both = like(c, 1 if s == k else 2)
                self._arrived(c, site, both)
                self._left(c, site, both)

            steps.append(Step(start, finish))
        return steps

    def _direct(self, axis, rows, lanes, send_ref, own, rx, total):
        n = DIMS[axis]
        site = self._site()

        def start(c):
            for by in range(1, n):
                t = self.torus.shifted(axis, by)
                self._copy(c, site, send_ref(c, t), rx(c).at[by - 1], axis, by)

        def finish(c):
            self._arrived(c, site, rx(c))

            def add(r0, size):
                value = own(c, r0, size)
                for i in range(n - 1):
                    value = value + rx(c)[i, pl.ds(r0, size), :].astype(F32)
                total(c, r0, size, value)

            rows_loop(rows, lanes, add)
            self._left(c, site, rx(c))

        return [Step(start, finish)]

    def _direct_gather(self, axis, mine, like):
        n = DIMS[axis]
        site = self._site()

        def start(c):
            for by in range(1, n):
                self._copy(c, site, mine(c), mine(c), axis, by)

        def finish(c):
            self._arrived(c, site, like(c))
            self._left(c, site, like(c))

        return [Step(start, finish)]

    def _steps(self):
        a1, a2, a3 = self.order
        rows1, lanes2, rows3 = self.rows1, self.lanes2, self.rows3
        at = [self.torus.at[a] for a in self.order]
        chunk = self.chunk

        def block1(c, t, r0, n):
            return chunk(c).at[ds(t * rows1 + r0, n, 16), :]

        def own1(c, t, r0, n):
            return chunk(c)[ds(t * rows1 + r0, n, 16), :].astype(F32)

        def total1(c, r0, n, value):
            at_ = ds(r0, n, 16)
            self.p32[at_, :] = value
            self.pb[at_, :] = value.astype(BF16)

        steps = self._chain(a1, rows1, BLOCK, block1, own1, lambda c, s: self.rx1.at[lax.rem(c, SLOTS), s], total1)

        def own2(c, t, r0, n):
            return self.p32[ds(r0, n, 16), ds(t * lanes2, lanes2)]

        def total2(c, r0, n, value):
            at_ = ds(r0, n, 16)
            self.r32[at_, :] = value
            self.rb[at_, :] = value.astype(BF16)

        if self.chained:
            steps += self._chain(
                a2,
                rows1,
                lanes2,
                lambda c, t, r0, n: self.pb.at[ds(r0, n, 16), ds(t * lanes2, lanes2)],
                own2,
                lambda c, s: self.rx2.at[lax.rem(c, SLOTS), s],
                total2,
            )
        else:
            steps += self._direct(
                a2,
                rows1,
                lanes2,
                lambda c, t: self.pb.at[:, ds(t * lanes2, lanes2)],
                lambda c, r0, n: own2(c, at[1], r0, n),
                lambda c: self.rx2.at[lax.rem(c, SLOTS)],
                total2,
            )

        def final(c):
            return chunk(c).at[ds(at[0] * rows1 + at[2] * rows3, rows3, 16), ds(at[1] * lanes2, lanes2)]

        def total3(c, r0, n, value):
            final(c)[ds(r0, n, 16), :] = value.astype(BF16)

        steps += self._direct(
            a3,
            rows3,
            lanes2,
            lambda c, t: self.rb.at[ds(t * rows3, rows3, 16), :],
            lambda c, r0, n: self.r32[ds(at[2] * rows3 + r0, n, 16), :],
            lambda c: self.rx3.at[lax.rem(c, SLOTS)],
            total3,
        )
        steps += self._direct_gather(a3, final, lambda c: self.rx3.at[lax.rem(c, SLOTS)])

        def block2(c, t, r0, n):
            return chunk(c).at[ds(at[0] * rows1 + r0, n, 16), ds(t * lanes2, lanes2)]

        if self.chained:
            steps += self._chain_gather(a2, rows1, block2, lambda c, n: chunk(c).at[pl.ds(0, rows1), pl.ds(0, n * lanes2)])
        else:
            steps += self._direct_gather(a2, lambda c: block2(c, at[1], 0, rows1), lambda c: self.rx2.at[lax.rem(c, SLOTS)])
        steps += self._chain_gather(a1, rows1, block1, lambda c, n: chunk(c).at[pl.ds(0, n * rows1), :])
        return steps

    @staticmethod
    def scratch(order, chained, chunks):
        n1, n2, n3 = (DIMS[a] for a in order)
        rows1, lanes2 = BLOCK // n1, BLOCK // n2
        rx2 = (chunks, n2 // 2, 2, rows1, lanes2) if chained else (chunks, n2 - 1, rows1, lanes2)
        return [
            pltpu.VMEM((chunks, n1 // 2, 2, rows1, BLOCK), BF16),
            pltpu.VMEM(rx2, BF16),
            pltpu.VMEM((chunks, n3 - 1, rows1 // n3, lanes2), BF16),
            pltpu.VMEM((rows1, BLOCK), F32),
            pltpu.VMEM((rows1, BLOCK), BF16),
            pltpu.VMEM((rows1, lanes2), F32),
            pltpu.VMEM((rows1, lanes2), BF16),
        ]

    @staticmethod
    def n_sites(order, chained):
        k1, k2 = DIMS[order[0]] // 2, DIMS[order[1]] // 2
        return 2 * k1 + (2 * k2 if chained else 2) + 2


DOWN, GATE, UP = range(3)
COLOURS = (((0, 1, 2), True), ((1, 0, 2), True), ((2, 0, 1), False))


def dot(a, b, dims=(((1,), (0,)), ((), ()))):
    return lax.dot_general(a, b, dims, preferred_element_type=F32)


def inverse_rms(wide):
    return lax.rsqrt(jnp.mean(wide * wide, -1, keepdims=True) + 1e-6)


def normed(h):
    wide = h.astype(F32)
    return (wide * inverse_rms(wide)).astype(BF16)


def sigmoid(x):
    return 0.5 * jnp.tanh(0.5 * x) + 0.5


def tiles(rows, size, body):
    def one(i, _):
        body(pl.ds(pl.multiple_of(i * size, size), size))
        return 0

    lax.fori_loop(0, rows // size, one, 0)


class Compute:
    def __init__(self, weights, states, dh, a, by, da):
        self.weights = weights
        self.states = states
        self.dh = dh
        self.a = a
        self.by = by
        self.da = da

    def forward(self, number):
        rows, blocks = self.a.shape[0], self.weights.shape[2]

        def body(at):
            h = self.states[number, at, :]
            a = normed(h)
            for block in range(blocks):
                for first in range(0, BLOCK, BLOCK // 2):
                    part = pl.ds(first, BLOCK // 2)
                    gate = dot(a, self.weights[GATE, number, block, :, part])
                    up = dot(a, self.weights[UP, number, block, :, part])
                    self.by[block, at, part] = (gate * sigmoid(gate) * up).astype(BF16)
            out = None
            for block in range(blocks):
                more = dot(self.by[block, at, :], self.weights[DOWN, number, block])
                out = more if out is None else out + more
            h = h + out.astype(BF16)
            self.states[number + 1, at, :] = h
            self.a[at, :] = normed(h)

        tiles(rows, min(TILE, rows), body)

    def back(self, number, block, tile):
        size = self.a.shape[0] // 4
        at = pl.ds(tile * size, size)
        for first in range(0, BLOCK, BLOCK // 2):
            part = pl.ds(first, BLOCK // 2)
            a = self.a[at, :]
            gate = dot(a, self.weights[GATE, number, block, :, part])
            up = dot(a, self.weights[UP, number, block, :, part])
            by = dot(self.dh[at, :], self.weights[DOWN, number, block, part, :], NT).astype(BF16).astype(F32)
            s = sigmoid(gate)
            silu = gate * s
            self.by[DOWN, at, part] = (silu * up).astype(BF16)
            self.by[GATE, at, part] = (by * up * (s + silu * (1.0 - s))).astype(BF16)
            self.by[UP, at, part] = (by * silu).astype(BF16)

    def gradient(self, which, into):
        if which == DOWN:
            into[...] = dot(self.by[DOWN], self.dh[...], TN).astype(BF16)
        else:
            into[...] = dot(self.a[...], self.by[which], TN).astype(BF16)

    def inputs(self, number, block, tile):
        size = self.a.shape[0] // 2
        at = pl.ds(tile * size, size)
        part = dot(self.by[GATE, at, :], self.weights[GATE, number, block], NT)
        part = part + dot(self.by[UP, at, :], self.weights[UP, number, block], NT)
        self.da[at, :] = jnp.where(block == 0, 0.0, self.da[at, :]) + part

    def below(self, number):
        rows = self.a.shape[0]

        def body(at):
            wide = self.states[number, at, :].astype(F32)
            by = self.da[at, :].astype(BF16).astype(F32)
            scale = inverse_rms(wide)
            by = by * scale - wide * (scale * scale * scale * jnp.mean(by * wide, -1, keepdims=True))
            self.dh[at, :] = self.dh[at, :] + by.astype(BF16)
            self.a[at, :] = normed(self.states[number - 1, at, :])

        tiles(rows, min(256, rows), body)


def block_at(arrays, which, number, j, r0=0, n=BLOCK):
    if which == DOWN:
        return arrays[2].at[number, ds(j * BLOCK + r0, n), :]
    return arrays[which - 1].at[number, ds(r0, n), ds(j * BLOCK, BLOCK)]


def train_kernel(x, dy, *refs):
    weights, moments, (g, w, kept), refs = refs[:3], (refs[3:6], refs[6:9]), refs[9:12], refs[12:]
    (states, dh, a, by, da), scratch = refs[:5], refs[5:]
    scratch, (send_sems, recv_sems, in_sems) = scratch[:-3], scratch[-3:]
    _, layers, blocks, _, _ = w.shape
    chunks = layers * blocks
    assert layers == 2
    torus = Torus()
    wait_barrier = torus.barrier()
    early = [(x.at[0], states.at[0])]
    early += [(block_at(weights, which, 0, j), w.at[which, 0, j]) for j in range(blocks) for which in (GATE, UP, DOWN)]
    late = [(block_at(weights, which, 1, j), w.at[which, 1, j]) for j in range(blocks) for which in (GATE, UP, DOWN)]
    late.append((dy.at[0], dh))
    idle = [
        (block_at(moments[k], which, layers - 1, j), kept.at[k, which, j])
        for k in range(2)
        for which in range(3)
        for j in range(blocks)
    ]

    def copies(pairs, group):
        return [pltpu.make_async_copy(src, dst, in_sems.at[group, i]) for i, (src, dst) in enumerate(pairs)]

    early, late, idle = (copies(pairs, group) for group, pairs in enumerate((early, late, idle)))
    for copy in (*early, *late):
        copy.start()
    compute = Compute(w, states, dh, a, by, da)
    for copy in early:
        copy.wait()
    compute.forward(0)
    for copy in late:
        copy.wait()
    for copy in idle:
        copy.start()
    wait_barrier()

    sites, exchanges = [0], []
    for k, (order, chained) in enumerate(COLOURS):
        rx, temporary = scratch[7 * k : 7 * k + 3], scratch[7 * k + 3 : 7 * k + 7]
        exchanges.append(Exchange(torus, order, chained, lambda c, k=k: g.at[c, k], rx, *temporary, (send_sems, recv_sems), sites))

    def stage(c, k, s):
        steps = exchanges[k].steps
        if s:
            steps[s - 1].finish(c)
        if s < len(steps):
            steps[s].start(c)

    def work(name, c):
        number, block = layers - 1 - lax.div(c, blocks), lax.rem(c, blocks)
        if name == "below":

            @pl.when((c > 0) & (c < chunks) & (block == 0))
            def _():
                compute.below(number + 1)

            return
        what, _, tile = name.partition(" ")

        @pl.when(c < (chunks - blocks if what == "inputs" else chunks))
        def _():
            if what == "back":
                compute.back(number, block, int(tile))
            elif what == "inputs":
                compute.inputs(number, block, int(tile))
            else:
                which = ("down", "gate", "up").index(what)
                compute.gradient(which, g.at[c, which])

    lags = [item[2] for item in PERIOD if not isinstance(item, str)]

    def body(period, _):
        i = 0
        while i < len(PERIOD):
            if isinstance(PERIOD[i], str):
                work(PERIOD[i], period)
                i += 1
                continue
            j = i
            while j < len(PERIOD) and not isinstance(PERIOD[j], str) and PERIOD[j][2] == PERIOD[i][2]:
                j += 1
            c = period - PERIOD[i][2]

            @pl.when((c >= 0) & (c < chunks))
            def _(c=c, group=PERIOD[i:j]):
                for k, s, _ in group:
                    stage(c, k, s)

            i = j
        return 0

    lax.fori_loop(0, chunks + max(lags), body, 0)
    for copy in idle:
        copy.wait()


def gradients(x, dy, weights, moments):
    gate, up, down = weights
    layers, d, ff = gate.shape
    tokens = x.shape[1]
    chunks = layers * ff // BLOCK
    scratch = [
        pltpu.VMEM((layers, tokens, d), BF16),
        pltpu.VMEM((tokens, d), BF16),
        pltpu.VMEM((tokens, d), BF16),
        pltpu.VMEM((3, tokens, BLOCK), BF16),
        pltpu.VMEM((tokens, d), F32),
    ]
    n_sites = 0
    for order, chained in COLOURS:
        scratch += Exchange.scratch(order, chained, SLOTS)
        n_sites += Exchange.n_sites(order, chained)
    scratch += [pltpu.SemaphoreType.DMA((SLOTS, n_sites))] * 2 + [pltpu.SemaphoreType.DMA((3, 6 * ff // BLOCK))]
    out = [
        pltpu.VMEM((chunks, 3, BLOCK, BLOCK), BF16),
        pltpu.VMEM((3, layers, ff // BLOCK, BLOCK, BLOCK), BF16),
        pltpu.VMEM((2, 3, ff // BLOCK, BLOCK, BLOCK), F32),
    ]
    return pl.pallas_call(
        train_kernel,
        out_shape=out,
        in_specs=[pl.BlockSpec(memory_space=pltpu.HBM)] * 11,
        out_specs=[pl.BlockSpec(memory_space=pltpu.VMEM)] * len(out),
        scratch_shapes=scratch,
        compiler_params=pltpu.CompilerParams(collective_id=0, has_side_effects=True, vmem_limit_bytes=VMEM_LIMIT),
        name="gradients",
    )(x, dy, *weights, *moments)


def adamw(w, m, v, g):
    m = 0.9 * m + 0.1 * g
    v = 0.95 * v + 0.05 * g * g
    step = m * lax.rsqrt(v + 1e-8) + 0.1 * w
    return (w - 0.02 * step).astype(BF16), m, v


def adamw_kernel(g, w, kept, *refs):
    moments, new, refs = (refs[:3], refs[3:6]), (refs[6:9], refs[9:12], refs[12:15]), refs[15:]
    first, *staged, in_sems, out_sems = refs
    _, layers, blocks, _, _ = w.shape
    parts = BLOCK // PIECE

    def load(which, j):
        return [
            pltpu.make_async_copy(block_at(moments[k], which, 0, j), first.at[k, which, j], in_sems.at[k, which, j])
            for k in range(2)
        ]

    def save(number, slot, which, j, r0):
        return [
            pltpu.make_async_copy(staged[k].at[number, slot], block_at(new[k], which, number, j, r0, PIECE), out_sems.at[number, slot, k])
            for k in range(3)
        ]

    for which in range(3):
        for j in range(blocks):
            for copy in load(which, j):
                copy.start()

    for which in range(3):

        def one(i, _, which=which):
            j, r = lax.div(i, parts), lax.rem(i, parts)
            slot = lax.rem(i, OUTPUTS)

            @pl.when(r == 0)
            def _():
                for copy in load(which, j):
                    copy.wait()

            for number in reversed(range(layers)):

                @pl.when(which * blocks * parts + i >= OUTPUTS)
                def _(number=number):
                    for copy in save(number, slot, which, j, r * PIECE):
                        copy.wait()

                moment = kept if number else first
                for r0 in range(0, PIECE, STRIP):
                    rows = ds(r * PIECE + r0, STRIP)
                    grad = g[(layers - 1 - number) * blocks + j, which, rows, :].astype(F32)
                    now = adamw(w[which, number, j, rows, :].astype(F32), moment[0, which, j, rows, :], moment[1, which, j, rows, :], grad)
                    for k in range(3):
                        staged[k][number, slot, pl.ds(r0, STRIP), :] = now[k]
                for copy in save(number, slot, which, j, r * PIECE):
                    copy.start()
            return 0

        lax.fori_loop(0, blocks * parts, one, 0)
    for slot in range(OUTPUTS):
        for number in range(layers):
            for copy in save(number, slot, DOWN, 0, 0):
                copy.wait()


def update(g, w, kept, weights, moments):
    _, layers, blocks, _, _ = w.shape
    vmem, hbm = pl.BlockSpec(memory_space=pltpu.VMEM), pl.BlockSpec(memory_space=pltpu.HBM)
    return pl.pallas_call(
        adamw_kernel,
        out_shape=[jax.ShapeDtypeStruct(a.shape, BF16) for a in weights] + [jax.ShapeDtypeStruct(a.shape, F32) for a in moments],
        in_specs=[vmem] * 3 + [hbm] * 6,
        out_specs=[hbm] * 9,
        scratch_shapes=[
            pltpu.VMEM((2, 3, blocks, BLOCK, BLOCK), F32),
            *(pltpu.VMEM((layers, OUTPUTS, PIECE, BLOCK), dtype) for dtype in (BF16, F32, F32)),
            pltpu.SemaphoreType.DMA((2, 3, blocks)),
            pltpu.SemaphoreType.DMA((layers, OUTPUTS, 3)),
        ],
        compiler_params=pltpu.CompilerParams(vmem_limit_bytes=UPDATE_LIMIT),
        name="update",
    )(g, w, kept, *moments)


def solution(mesh):
    def step(x, dy, *arrays):
        weights, moments = arrays[:3], arrays[3:]
        there = gradients(x, dy, weights, moments)
        there = [pltpu.with_memory_space_constraint(a, pltpu.VMEM) for a in there]
        moments = [pltpu.with_memory_space_constraint(a, pltpu.HBM) for a in moments]
        return tuple(update(*there, weights, moments))

    return jax.shard_map(
        step,
        mesh=mesh,
        in_specs=(P(("rep", "dp"), None, None),) * 2 + (P(None, None, None),) * 9,
        out_specs=(P("rep", None, None),) * 9,
        check_vma=False,
    )
```

```python
import functools

import jax
import jax.numpy as jnp
from jax import lax
from jax.experimental import pallas as pl
from jax.experimental.pallas import tpu as pltpu
from jax.sharding import PartitionSpec as P

MESH = pl.DeviceIdType.MESH
DIMS = (4, 4, 8)
BLOCK = 512
TILE = 512
PIECE = 128
STRIP = 32
SLOTS = 3
OUTPUTS = 4
PERIOD = (
    "back 0",
    (0, 4, 2), (1, 7, 4), (0, 1, 1), (0, 9, 5),
    "back 1",
    (2, 2, 1), (2, 5, 2), (1, 9, 5), (0, 6, 3),
    "back 2",
    (1, 4, 2), (2, 11, 5),
    "back 3",
    (1, 2, 1), (0, 8, 4), (2, 8, 3),
    "up",
    (0, 2, 1), (2, 0, 0), (1, 6, 3), (2, 3, 1), (2, 6, 2),
    "gate",
    (1, 0, 0), (0, 5, 2),
    "down",
    (1, 8, 4), (1, 5, 2), (2, 10, 4), (0, 0, 0),
    "inputs 0",
    (0, 3, 1), (2, 12, 5), (2, 1, 0), (1, 10, 5), (2, 4, 1), (2, 7, 2),
    "inputs 1",
    (2, 9, 3), (1, 3, 1), (0, 7, 3), (0, 10, 5), (1, 1, 0),
)
VMEM_LIMIT = UPDATE_LIMIT = 29_200_000
TN = (((0,), (0,)), ((), ()))
NT = (((1,), (1,)), ((), ()))
BF16, F32 = jnp.bfloat16, jnp.float32


def ds(start, size, multiple=None):
    if isinstance(start, int):
        return pl.ds(start, size)
    return pl.ds(pl.multiple_of(start, multiple or size), size)


class Torus:
    def __init__(self):
        i = lax.axis_index("dp")
        nx, ny, nz = DIMS
        self.at = (lax.div(i, ny * nz), lax.rem(lax.div(i, nz), ny), lax.rem(i, nz))
        self._places, self._devices = {}, {}
        for axis, n in enumerate(DIMS):
            for by in range(n):
                self._places[axis, by] = place = lax.rem(self.at[axis] + by, n) if by else self.at[axis]
                to = list(self.at)
                to[axis] = place
                self._devices[axis, by] = (to[0] * ny + to[1]) * nz + to[2]

    def shifted(self, axis, by):
        return self._places[axis, by % DIMS[axis]]

    def device(self, axis, by):
        return {"dp": self._devices[axis, by % DIMS[axis]]}

    def barrier(self):
        sem = pltpu.get_barrier_semaphore()
        peers = [(axis, by) for axis in range(3) for by in range(1, DIMS[axis])]
        for axis, by in peers:
            pl.semaphore_signal(sem, inc=1, device_id=self.device(axis, by), device_id_type=MESH)
        return lambda: pl.semaphore_wait(sem, len(peers))


class Step:
    def __init__(self, start, finish):
        self.start, self.finish = start, finish


def rows_loop(rows, lanes, body):
    size = min(rows, 32 * 1024 // lanes)
    for r0 in range(0, rows, size):
        body(r0, min(size, rows - r0))


class Exchange:
    def __init__(self, torus, order, chained, far, chunk, rx, p32, pb, r32, rb, sems, sites):
        self.torus, self.order, self.chained = torus, order, chained
        self.chunk = chunk
        self.rx1, self.rx2, self.rx3 = rx
        self.p32, self.pb, self.r32, self.rb = p32, pb, r32, rb
        self.send_sems, self.recv_sems = sems
        self.sites = sites
        n1, n2, n3 = (DIMS[a] for a in order)
        self.rows1 = BLOCK // n1
        self.far = int(self.rows1 * far) // 16 * 16
        self.lanes2 = BLOCK // n2
        self.rows3 = self.rows1 // n3
        self.steps = self._steps()

    def _site(self):
        s = self.sites[0]
        self.sites[0] += 1
        return s

    def _copy(self, c, site, src, dst, axis, by):
        pltpu.make_async_remote_copy(
            src_ref=src,
            dst_ref=dst,
            send_sem=self.send_sems.at[c],
            recv_sem=self.recv_sems.at[lax.rem(c, SLOTS), site],
            device_id=self.torus.device(axis, by),
            device_id_type=MESH,
        ).start()

    @staticmethod
    def _blocks(ref):
        def rx(c, i, n=None):
            return ref.at[lax.rem(c, SLOTS), i if n is None else pl.ds(i, n)]

        return rx

    def _arrived(self, c, site, like):
        pltpu.make_async_copy(like, like, self.recv_sems.at[lax.rem(c, SLOTS), site]).wait()

    def _left(self, c, like):
        pltpu.make_async_copy(like, like, self.send_sems.at[c]).wait()

    def _chain(self, axis, rows, far, lanes, send_ref, own, rx, total):
        k = DIMS[axis] // 2
        ways = ((1, 0, (0, far), (far, rows - far)), (-1, 1, (far, rows - far), (0, far)))

        def got(c, s, w):
            return rx(c, 0 if s == 1 else 2 * s - 3 + w)

        steps = []
        for s in range(1, k + 1):
            site = self._site()

            def start(c, s=s, site=site):
                for way, w, mine, others in ways:
                    t = self.torus.shifted(axis, way * (k + 1 - s))
                    dst = got(c, s, w)
                    if s == 1:
                        self._copy(c, site, send_ref(c, t, *mine), dst.at[ds(*mine, 16), :], axis, way)
                    elif s == 2:
                        self._copy(c, site, got(c, 1, w).at[ds(*mine, 16), :], dst.at[ds(*mine, 16), :], axis, way)
                        self._copy(c, site, send_ref(c, t, *others), dst.at[ds(*others, 16), :], axis, way)
                    else:
                        self._copy(c, site, got(c, s - 1, w), dst, axis, way)

            def finish(c, s=s, site=site):
                like = rx(c, 0) if s == 1 else rx(c, 2 * s - 3, 2)
                self._arrived(c, site, like)
                if s < k:
                    for way, w, mine, _ in ways:
                        t = self.torus.shifted(axis, way * (k - s))
                        first, count = mine if s == 1 else (0, rows)
                        here = got(c, s, w)

                        def add(r0, size, here=here, t=t, first=first):
                            at = pl.ds(first + r0, size)
                            here[at, :] = (here[at, :].astype(F32) + own(c, t, first + r0, size)).astype(BF16)

                        rows_loop(count, lanes, add)
                else:
                    me = self.torus.shifted(axis, 0)
                    for _, here, (first, count), _ in ways:

                        def add(r0, size, here=here, first=first):
                            at = pl.ds(first + r0, size)
                            value = own(c, me, first + r0, size)
                            for w in range(2):
                                if k > 1 or w == here:
                                    value = value + got(c, s, w)[at, :].astype(F32)
                            total(c, first + r0, size, value)

                        rows_loop(count, lanes, add)
                self._left(c, like)

            steps.append(Step(start, finish))
        return steps

    def _chain_gather(self, axis, rows, far, block, like):
        k = DIMS[axis] // 2
        ways = ((1, (0, far)), (-1, (far, rows - far)))
        steps = []
        for s in range(1, k + 1):
            site = self._site()

            def start(c, s=s, site=site):
                for way, mine in ways:
                    t = self.torus.shifted(axis, -way * (s - 1))
                    ref = block(c, t, *mine) if s == k else block(c, t, 0, rows)
                    self._copy(c, site, ref, ref, axis, way)

            def finish(c, s=s, site=site):
                both = like(c, 1 if s == k else 2)
                self._arrived(c, site, both)
                self._left(c, both)

            steps.append(Step(start, finish))
        return steps

    def _direct(self, axis, rows, lanes, send_ref, own, rx, total):
        n = DIMS[axis]
        site = self._site()

        def start(c):
            for by in range(1, n):
                t = self.torus.shifted(axis, by)
                self._copy(c, site, send_ref(c, t), rx(c).at[by - 1], axis, by)

        def finish(c):
            self._arrived(c, site, rx(c))

            def add(r0, size):
                value = own(c, r0, size)
                for i in range(n - 1):
                    value = value + rx(c)[i, pl.ds(r0, size), :].astype(F32)
                total(c, r0, size, value)

            rows_loop(rows, lanes, add)
            self._left(c, rx(c))

        return [Step(start, finish)]

    def _direct_gather(self, axis, mine, like):
        n = DIMS[axis]
        site = self._site()

        def start(c):
            for by in range(1, n):
                self._copy(c, site, mine(c), mine(c), axis, by)

        def finish(c):
            self._arrived(c, site, like(c))
            self._left(c, like(c))

        return [Step(start, finish)]

    def _steps(self):
        a1, a2, a3 = self.order
        rows1, lanes2, rows3 = self.rows1, self.lanes2, self.rows3
        at = [self.torus.at[a] for a in self.order]
        chunk = self.chunk

        def block1(c, t, r0, n):
            return chunk(c).at[ds(t * rows1 + r0, n, 16), :]

        def own1(c, t, r0, n):
            return chunk(c)[ds(t * rows1 + r0, n, 16), :].astype(F32)

        def total1(c, r0, n, value):
            at_ = ds(r0, n, 16)
            self.p32[at_, :] = value
            self.pb[at_, :] = value.astype(BF16)

        steps = self._chain(a1, rows1, self.far, BLOCK, block1, own1, self._blocks(self.rx1), total1)

        def own2(c, t, r0, n):
            return self.p32[ds(r0, n, 16), ds(t * lanes2, lanes2)]

        def total2(c, r0, n, value):
            at_ = ds(r0, n, 16)
            self.r32[at_, :] = value
            self.rb[at_, :] = value.astype(BF16)

        if self.chained:
            steps += self._chain(
                a2,
                rows1,
                rows1 // 2,
                lanes2,
                lambda c, t, r0, n: self.pb.at[ds(r0, n, 16), ds(t * lanes2, lanes2)],
                own2,
                self._blocks(self.rx2),
                total2,
            )
        else:
            steps += self._direct(
                a2,
                rows1,
                lanes2,
                lambda c, t: self.pb.at[:, ds(t * lanes2, lanes2)],
                lambda c, r0, n: own2(c, at[1], r0, n),
                lambda c: self.rx2.at[lax.rem(c, SLOTS)],
                total2,
            )

        def final(c):
            return chunk(c).at[ds(at[0] * rows1 + at[2] * rows3, rows3, 16), ds(at[1] * lanes2, lanes2)]

        def total3(c, r0, n, value):
            final(c)[ds(r0, n, 16), :] = value.astype(BF16)

        steps += self._direct(
            a3,
            rows3,
            lanes2,
            lambda c, t: self.rb.at[ds(t * rows3, rows3, 16), :],
            lambda c, r0, n: self.r32[ds(at[2] * rows3 + r0, n, 16), :],
            lambda c: self.rx3.at[lax.rem(c, SLOTS)],
            total3,
        )
        steps += self._direct_gather(a3, final, lambda c: self.rx3.at[lax.rem(c, SLOTS)])

        def block2(c, t, r0, n):
            return chunk(c).at[ds(at[0] * rows1 + r0, n, 16), ds(t * lanes2, lanes2)]

        if self.chained:
            steps += self._chain_gather(a2, rows1, rows1 // 2, block2, lambda c, n: chunk(c).at[pl.ds(0, rows1), pl.ds(0, n * lanes2)])
        else:
            steps += self._direct_gather(a2, lambda c: block2(c, at[1], 0, rows1), lambda c: self.rx2.at[lax.rem(c, SLOTS)])
        steps += self._chain_gather(a1, rows1, self.far, block1, lambda c, n: chunk(c).at[pl.ds(0, n * rows1), :])
        return steps

    @staticmethod
    def scratch(order, chained, chunks):
        n1, n2, n3 = (DIMS[a] for a in order)
        rows1, lanes2 = BLOCK // n1, BLOCK // n2
        rx2 = (chunks, n2 - 1, rows1, lanes2) if chained else (chunks, n2 - 1, rows1, lanes2)
        return [
            pltpu.VMEM((chunks, n1 - 1, rows1, BLOCK), BF16),
            pltpu.VMEM(rx2, BF16),
            pltpu.VMEM((chunks, n3 - 1, rows1 // n3, lanes2), BF16),
            pltpu.VMEM((rows1, BLOCK), F32),
            pltpu.VMEM((rows1, BLOCK), BF16),
            pltpu.VMEM((rows1, lanes2), F32),
            pltpu.VMEM((rows1, lanes2), BF16),
        ]

    @staticmethod
    def n_sites(order, chained):
        k1, k2 = DIMS[order[0]] // 2, DIMS[order[1]] // 2
        return 2 * k1 + (2 * k2 if chained else 2) + 2


DOWN, GATE, UP = range(3)
COLOURS = (((0, 1, 2), True, 0.375), ((1, 0, 2), True, 0.5), ((2, 0, 1), False, 0.25))


def dot(a, b, dims=(((1,), (0,)), ((), ()))):
    return lax.dot_general(a, b, dims, preferred_element_type=F32)


def inverse_rms(wide):
    return lax.rsqrt(jnp.mean(wide * wide, -1, keepdims=True) + 1e-6)


def normed(h):
    wide = h.astype(F32)
    return (wide * inverse_rms(wide)).astype(BF16)


def sigmoid(x):
    return 0.5 * jnp.tanh(0.5 * x) + 0.5


class Compute:
    def __init__(self, weights, states, dh, a, by, da):
        self.weights = weights
        self.states = states
        self.dh = dh
        self.a = a
        self.by = by
        self.da = da

    def forward(self, wait):
        rows, blocks = self.a.shape[0], self.weights.shape[2]
        size = min(TILE, rows)

        def tile(at, wait):
            h = self.states[0, at, :]
            a = normed(h)
            for block in range(blocks):
                wait("in", block)
                for first in range(0, BLOCK, BLOCK // 2):
                    part = pl.ds(first, BLOCK // 2)
                    gate = dot(a, self.weights[GATE, 0, block, :, part])
                    up = dot(a, self.weights[UP, 0, block, :, part])
                    self.by[block, at, part] = (gate * sigmoid(gate) * up).astype(BF16)
            wait("out", 0)
            out = None
            for block in range(blocks):
                more = dot(self.by[block, at, :], self.weights[DOWN, 0, block])
                out = more if out is None else out + more
            h = h + out.astype(BF16)
            self.states[1, at, :] = h
            self.a[at, :] = normed(h)

        wait("x", 0)
        tile(pl.ds(0, size), wait)
        wait("x", 1)

        def one(i, _):
            tile(pl.ds(pl.multiple_of(i * size, size), size), lambda what, i: None)
            return 0

        lax.fori_loop(1, rows // size, one, 0)

    def back(self, number, block, tile):
        size = self.a.shape[0] // 4
        at = pl.ds(tile * size, size)
        for first in range(0, BLOCK, BLOCK // 2):
            part = pl.ds(first, BLOCK // 2)
            a = self.a[at, :]
            gate = dot(a, self.weights[GATE, number, block, :, part])
            up = dot(a, self.weights[UP, number, block, :, part])
            by = dot(self.dh[at, :], self.weights[DOWN, number, block, part, :], NT).astype(BF16).astype(F32)
            s = sigmoid(gate)
            silu = gate * s
            self.by[DOWN, at, part] = (silu * up).astype(BF16)
            self.by[GATE, at, part] = (by * up * (s + silu * (1.0 - s))).astype(BF16)
            self.by[UP, at, part] = (by * silu).astype(BF16)

    def gradient(self, which, into):
        if which == DOWN:
            into[...] = dot(self.by[DOWN], self.dh[...], TN).astype(BF16)
        else:
            into[...] = dot(self.a[...], self.by[which], TN).astype(BF16)

    def _inputs(self, block, at):
        part = dot(self.by[GATE, at, :], self.weights[GATE, 1, block], NT)
        return part + dot(self.by[UP, at, :], self.weights[UP, 1, block], NT)

    def inputs(self, block, tile):
        size = self.a.shape[0] // 2
        at = pl.ds(tile * size, size)
        self.da[at, :] = jnp.where(block == 0, 0.0, self.da[at, :]) + self._inputs(block, at)

    def below(self, tile):
        size = self.a.shape[0] // 8

        def one(i, _):
            at = pl.ds(pl.multiple_of(i * size, size), size)
            by = (self.da[at, :] + self._inputs(self.weights.shape[2] - 1, at)).astype(BF16).astype(F32)
            wide = self.states[1, at, :].astype(F32)
            scale = inverse_rms(wide)
            by = by * scale - wide * (scale * scale * scale * jnp.mean(by * wide, -1, keepdims=True))
            self.dh[at, :] = self.dh[at, :] + by.astype(BF16)
            self.a[at, :] = normed(self.states[0, at, :])
            return 0

        lax.fori_loop(4 * tile, 4 * tile + 4, one, 0)


def block_at(arrays, which, number, j, r0=0, n=BLOCK):
    if which == DOWN:
        return arrays[2].at[number, ds(j * BLOCK + r0, n), :]
    return arrays[which - 1].at[number, ds(r0, n), ds(j * BLOCK, BLOCK)]


def train_kernel(x, dy, *refs):
    weights, moments, (g, w, kept), refs = refs[:3], (refs[3:6], refs[6:9]), refs[9:12], refs[12:]
    (states, dh, a, by, da), scratch = refs[:5], refs[5:]
    scratch, (send_sems, recv_sems, in_sems) = scratch[:-3], scratch[-3:]
    _, layers, blocks, _, _ = w.shape
    chunks = layers * blocks
    assert layers == 2
    torus = Torus()
    wait_barrier = torus.barrier()
    size = min(TILE, dh.shape[0])

    def weight(which, number, j):
        return block_at(weights, which, number, j), w.at[which, number, j]

    first = x.at[0, pl.ds(0, size)], states.at[0, pl.ds(0, size)]
    rest = x.at[0, pl.ds(size, x.shape[1] - size)], states.at[0, pl.ds(size, x.shape[1] - size)]
    groups = {("x", 0): ([first], first[1])}
    for j in range(blocks):
        groups["in", j] = [weight(which, 0, j) for which in (GATE, UP)], w.at[pl.ds(GATE, 2), 0, j]
        if j == 0:
            groups["out", 0] = [weight(DOWN, 0, i) for i in range(blocks)], w.at[DOWN, 0]
    groups["x", 1] = [rest], rest[1]
    groups["late", 0] = [weight(which, 1, j) for j in range(blocks) for which in range(3)], w.at[:, 1]
    groups["late", 1] = [(dy.at[0], dh)], dh
    idle = [(block_at(moments[k], i, layers - 1, j), kept.at[k, i, j]) for k in range(2) for i in range(3) for j in range(blocks)]
    groups["idle", 0] = idle, kept
    sem_of = {key: i for i, key in enumerate(groups)}

    def begin(key):
        for src, dst in groups[key][0]:
            pltpu.make_async_copy(src, dst, in_sems.at[sem_of[key]]).start()

    def wait(*key):
        like = groups[key][1]
        pltpu.make_async_copy(like, like, in_sems.at[sem_of[key]]).wait()

    for key in groups:
        if key[0] != "idle":
            begin(key)
    compute = Compute(w, states, dh, a, by, da)
    compute.forward(wait)
    wait("late", 0)
    wait("late", 1)
    begin(("idle", 0))
    wait_barrier()

    sites, exchanges = [0], []
    for k, (order, chained, far) in enumerate(COLOURS):
        rx, temporary = scratch[7 * k : 7 * k + 3], scratch[7 * k + 3 : 7 * k + 7]
        sems = send_sems.at[k], recv_sems
        exchanges.append(Exchange(torus, order, chained, far, lambda c, k=k: g.at[c, k], rx, *temporary, sems, sites))

    def stage(c, k, s):
        steps = exchanges[k].steps
        if s:
            steps[s - 1].finish(c)
        if s < len(steps):
            steps[s].start(c)

    def work(name, c):
        number, block = layers - 1 - lax.div(c, blocks), lax.rem(c, blocks)
        what, _, tile = name.partition(" ")
        if what == "inputs":

            @pl.when(c < blocks - 1)
            def _():
                compute.inputs(block, int(tile))

            @pl.when(c == blocks - 1)
            def _():
                compute.below(int(tile))

            return

        @pl.when(c < chunks)
        def _():
            if what == "back":
                compute.back(number, block, int(tile))
            else:
                which = ("down", "gate", "up").index(what)
                compute.gradient(which, g.at[c, which])

    lags = [item[2] for item in PERIOD if not isinstance(item, str)]

    def body(period, _):
        i = 0
        while i < len(PERIOD):
            if isinstance(PERIOD[i], str):
                work(PERIOD[i], period)
                i += 1
                continue
            j = i
            while j < len(PERIOD) and not isinstance(PERIOD[j], str) and PERIOD[j][2] == PERIOD[i][2]:
                j += 1
            c = period - PERIOD[i][2]

            @pl.when((c >= 0) & (c < chunks))
            def _(c=c, group=PERIOD[i:j]):
                for k, s, _ in group:
                    stage(c, k, s)

            i = j
        return 0

    lax.fori_loop(0, chunks + max(lags), body, 0)
    wait("idle", 0)


def gradients(x, dy, weights, moments):
    gate, up, down = weights
    layers, d, ff = gate.shape
    tokens = x.shape[1]
    chunks = layers * ff // BLOCK
    scratch = [
        pltpu.VMEM((layers, tokens, d), BF16),
        pltpu.VMEM((tokens, d), BF16),
        pltpu.VMEM((tokens, d), BF16),
        pltpu.VMEM((3, tokens, BLOCK), BF16),
        pltpu.VMEM((tokens, d), F32),
    ]
    n_sites = 0
    for order, chained, _ in COLOURS:
        scratch += Exchange.scratch(order, chained, SLOTS)
        n_sites += Exchange.n_sites(order, chained)
    scratch += [pltpu.SemaphoreType.DMA((len(COLOURS), chunks)), pltpu.SemaphoreType.DMA((SLOTS, n_sites)), pltpu.SemaphoreType.DMA((11,))]
    out = [
        pltpu.VMEM((chunks, 3, BLOCK, BLOCK), BF16),
        pltpu.VMEM((3, layers, ff // BLOCK, BLOCK, BLOCK), BF16),
        pltpu.VMEM((2, 3, ff // BLOCK, BLOCK, BLOCK), F32),
    ]
    return pl.pallas_call(
        train_kernel,
        out_shape=out,
        in_specs=[pl.BlockSpec(memory_space=pltpu.HBM)] * 11,
        out_specs=[pl.BlockSpec(memory_space=pltpu.VMEM)] * len(out),
        scratch_shapes=scratch,
        compiler_params=pltpu.CompilerParams(collective_id=0, has_side_effects=True, vmem_limit_bytes=VMEM_LIMIT),
        name="gradients",
    )(x, dy, *weights, *moments)


def adamw(w, m, v, g):
    m = 0.9 * m + 0.1 * g
    v = 0.95 * v + 0.05 * g * g
    step = m * lax.rsqrt(v + 1e-8) + 0.1 * w
    return (w - 0.02 * step).astype(BF16), m, v


def adamw_kernel(g, w, kept, *refs):
    moments, new, refs = (refs[:3], refs[3:6]), (refs[6:9], refs[9:12], refs[12:15]), refs[15:]
    first, *staged, in_sems, out_sems = refs
    _, layers, blocks, _, _ = w.shape
    parts = BLOCK // PIECE

    def load(which, j):
        return [
            pltpu.make_async_copy(block_at(moments[k], which, 0, j), first.at[k, which, j], in_sems.at[k, which, j])
            for k in range(2)
        ]

    def save(number, slot, which, j, r0):
        return [
            pltpu.make_async_copy(staged[k].at[number, slot], block_at(new[k], which, number, j, r0, PIECE), out_sems.at[number, slot, k])
            for k in range(3)
        ]

    for which in range(3):
        for j in range(blocks):
            for copy in load(which, j):
                copy.start()

    for which in range(3):

        def one(i, _, which=which):
            j, r = lax.div(i, parts), lax.rem(i, parts)
            slot = lax.rem(i, OUTPUTS)

            @pl.when(r == 0)
            def _():
                for copy in load(which, j):
                    copy.wait()

            for number in reversed(range(layers)):

                @pl.when(which * blocks * parts + i >= OUTPUTS)
                def _(number=number):
                    for copy in save(number, slot, which, j, r * PIECE):
                        copy.wait()

                moment = kept if number else first
                for r0 in range(0, PIECE, STRIP):
                    rows = ds(r * PIECE + r0, STRIP)
                    grad = g[(layers - 1 - number) * blocks + j, which, rows, :].astype(F32)
                    now = adamw(w[which, number, j, rows, :].astype(F32), moment[0, which, j, rows, :], moment[1, which, j, rows, :], grad)
                    for k in range(3):
                        staged[k][number, slot, pl.ds(r0, STRIP), :] = now[k]
                for copy in save(number, slot, which, j, r * PIECE):
                    copy.start()
            return 0

        lax.fori_loop(0, blocks * parts, one, 0)
    for slot in range(OUTPUTS):
        for number in range(layers):
            for copy in save(number, slot, DOWN, 0, 0):
                copy.wait()


def update(g, w, kept, weights, moments):
    _, layers, blocks, _, _ = w.shape
    vmem, hbm = pl.BlockSpec(memory_space=pltpu.VMEM), pl.BlockSpec(memory_space=pltpu.HBM)
    return pl.pallas_call(
        adamw_kernel,
        out_shape=[jax.ShapeDtypeStruct(a.shape, BF16) for a in weights] + [jax.ShapeDtypeStruct(a.shape, F32) for a in moments],
        in_specs=[vmem] * 3 + [hbm] * 6,
        out_specs=[hbm] * 9,
        scratch_shapes=[
            pltpu.VMEM((2, 3, blocks, BLOCK, BLOCK), F32),
            *(pltpu.VMEM((layers, OUTPUTS, PIECE, BLOCK), dtype) for dtype in (BF16, F32, F32)),
            pltpu.SemaphoreType.DMA((2, 3, blocks)),
            pltpu.SemaphoreType.DMA((layers, OUTPUTS, 3)),
        ],
        compiler_params=pltpu.CompilerParams(vmem_limit_bytes=UPDATE_LIMIT),
        name="update",
    )(g, w, kept, *moments)


def solution(mesh):
    def step(x, dy, *arrays):
        weights, moments = arrays[:3], arrays[3:]
        there = gradients(x, dy, weights, moments)
        there = [pltpu.with_memory_space_constraint(a, pltpu.VMEM) for a in there]
        moments = [pltpu.with_memory_space_constraint(a, pltpu.HBM) for a in moments]
        return tuple(update(*there, weights, moments))

    return jax.shard_map(
        step,
        mesh=mesh,
        in_specs=(P(("rep", "dp"), None, None),) * 2 + (P(None, None, None),) * 9,
        out_specs=(P("rep", None, None),) * 9,
        check_vma=False,
    )
```

```python
import functools

import jax
import jax.numpy as jnp
from jax import lax
from jax.experimental import pallas as pl
from jax.experimental.pallas import tpu as pltpu
from jax.sharding import PartitionSpec as P

MESH = pl.DeviceIdType.MESH
DIMS = (4, 4, 8)
BLOCK = 512
LAST = "down"
KEPT = 14
PIECE = 128
STRIP = 32
SLOTS = 3
OUTPUTS = 8
PERIOD = (
    "back 0",
    (0, 4, 2), (1, 7, 4), (0, 1, 1), (0, 9, 5),
    "back 1",
    (2, 2, 1), (2, 5, 2), (1, 9, 5), (0, 6, 3),
    "back 2",
    (1, 4, 2), (2, 11, 5),
    "back 3",
    (1, 2, 1), (0, 8, 4), (2, 8, 3),
    "up",
    (0, 2, 1), (2, 0, 0), (1, 6, 3), (2, 3, 1), (2, 6, 2),
    "gate",
    (1, 0, 0), (0, 5, 2),
    "down",
    (1, 8, 4), (1, 5, 2), (2, 10, 4), (0, 0, 0),
    "inputs 0",
    (0, 3, 1), (2, 12, 5), (2, 1, 0), (1, 10, 5), (2, 4, 1), (2, 7, 2),
    "inputs 1",
    (2, 9, 3), (1, 3, 1), (0, 7, 3), (0, 10, 5), (1, 1, 0),
)
VMEM_LIMIT = UPDATE_LIMIT = 16_700_000
TN = (((0,), (0,)), ((), ()))
NT = (((1,), (1,)), ((), ()))
BF16, F32 = jnp.bfloat16, jnp.float32


def ds(start, size, multiple=None):
    if isinstance(start, int):
        return pl.ds(start, size)
    return pl.ds(pl.multiple_of(start, multiple or size), size)


class Torus:
    def __init__(self):
        i = lax.axis_index("dp")
        nx, ny, nz = DIMS
        self.at = (lax.div(i, ny * nz), lax.rem(lax.div(i, nz), ny), lax.rem(i, nz))
        self._places, self._devices = {}, {}
        for axis, n in enumerate(DIMS):
            for by in range(n):
                self._places[axis, by] = place = lax.rem(self.at[axis] + by, n) if by else self.at[axis]
                to = list(self.at)
                to[axis] = place
                self._devices[axis, by] = (to[0] * ny + to[1]) * nz + to[2]

    def shifted(self, axis, by):
        return self._places[axis, by % DIMS[axis]]

    def device(self, axis, by):
        return {"dp": self._devices[axis, by % DIMS[axis]]}

    def barrier(self):
        sem = pltpu.get_barrier_semaphore()
        peers = [(axis, by) for axis in range(3) for by in range(1, DIMS[axis])]
        for axis, by in peers:
            pl.semaphore_signal(sem, inc=1, device_id=self.device(axis, by), device_id_type=MESH)
        return lambda: pl.semaphore_wait(sem, len(peers))


class Step:
    def __init__(self, start, finish):
        self.start, self.finish = start, finish


def rows_loop(rows, lanes, body):
    size = min(rows, 32 * 1024 // lanes)
    for r0 in range(0, rows, size):
        body(r0, min(size, rows - r0))


class Exchange:
    def __init__(self, torus, order, chained, far, chunk, rx, p32, pb, r32, rb, sems, sites):
        self.torus, self.order, self.chained = torus, order, chained
        self.chunk = chunk
        self.rx1, self.rx2, self.rx3 = rx
        self.p32, self.pb, self.r32, self.rb = p32, pb, r32, rb
        self.send_sems, self.recv_sems = sems
        self.sites = sites
        n1, n2, n3 = (DIMS[a] for a in order)
        self.rows1 = BLOCK // n1
        self.far = int(self.rows1 * far) // 16 * 16
        self.lanes2 = BLOCK // n2
        self.rows3 = self.rows1 // n3
        self.steps = self._steps()

    def _site(self):
        s = self.sites[0]
        self.sites[0] += 1
        return s

    def _copy(self, c, site, src, dst, axis, by):
        pltpu.make_async_remote_copy(
            src_ref=src,
            dst_ref=dst,
            send_sem=self.send_sems.at[c],
            recv_sem=self.recv_sems.at[lax.rem(c, SLOTS), site],
            device_id=self.torus.device(axis, by),
            device_id_type=MESH,
        ).start()

    @staticmethod
    def _blocks(ref):
        def rx(c, i, n=None):
            return ref.at[lax.rem(c, SLOTS), i if n is None else pl.ds(i, n)]

        return rx

    def _arrived(self, c, site, like):
        pltpu.make_async_copy(like, like, self.recv_sems.at[lax.rem(c, SLOTS), site]).wait()

    def _left(self, c, like):
        pltpu.make_async_copy(like, like, self.send_sems.at[c]).wait()

    def _chain(self, axis, rows, far, lanes, send_ref, own, rx, total):
        k = DIMS[axis] // 2
        ways = ((1, 0, (0, far), (far, rows - far)), (-1, 1, (far, rows - far), (0, far)))

        def got(c, s, w):
            return rx(c, 0 if s == 1 else 2 * s - 3 + w)

        steps = []
        for s in range(1, k + 1):
            site = self._site()

            def start(c, s=s, site=site):
                for way, w, mine, others in ways:
                    t = self.torus.shifted(axis, way * (k + 1 - s))
                    dst = got(c, s, w)
                    if s == 1:
                        self._copy(c, site, send_ref(c, t, *mine), dst.at[ds(*mine, 16), :], axis, way)
                    elif s == 2:
                        self._copy(c, site, got(c, 1, w).at[ds(*mine, 16), :], dst.at[ds(*mine, 16), :], axis, way)
                        self._copy(c, site, send_ref(c, t, *others), dst.at[ds(*others, 16), :], axis, way)
                    else:
                        self._copy(c, site, got(c, s - 1, w), dst, axis, way)

            def finish(c, s=s, site=site):
                like = rx(c, 0) if s == 1 else rx(c, 2 * s - 3, 2)
                self._arrived(c, site, like)
                if s < k:
                    for way, w, mine, _ in ways:
                        t = self.torus.shifted(axis, way * (k - s))
                        first, count = mine if s == 1 else (0, rows)
                        here = got(c, s, w)

                        def add(r0, size, here=here, t=t, first=first):
                            at = pl.ds(first + r0, size)
                            here[at, :] = (here[at, :].astype(F32) + own(c, t, first + r0, size)).astype(BF16)

                        rows_loop(count, lanes, add)
                else:
                    me = self.torus.shifted(axis, 0)
                    for _, here, (first, count), _ in ways:

                        def add(r0, size, here=here, first=first):
                            at = pl.ds(first + r0, size)
                            value = own(c, me, first + r0, size)
                            for w in range(2):
                                if k > 1 or w == here:
                                    value = value + got(c, s, w)[at, :].astype(F32)
                            total(c, first + r0, size, value)

                        rows_loop(count, lanes, add)
                self._left(c, like)

            steps.append(Step(start, finish))
        return steps

    def _chain_gather(self, axis, rows, far, block, like):
        k = DIMS[axis] // 2
        ways = ((1, (0, far)), (-1, (far, rows - far)))
        steps = []
        for s in range(1, k + 1):
            site = self._site()

            def start(c, s=s, site=site):
                for way, mine in ways:
                    t = self.torus.shifted(axis, -way * (s - 1))
                    ref = block(c, t, *mine) if s == k else block(c, t, 0, rows)
                    self._copy(c, site, ref, ref, axis, way)

            def finish(c, s=s, site=site):
                both = like(c, 1 if s == k else 2)
                self._arrived(c, site, both)
                self._left(c, both)

            steps.append(Step(start, finish))
        return steps

    def _direct(self, axis, rows, lanes, send_ref, own, rx, total):
        n = DIMS[axis]
        site = self._site()

        def start(c):
            for by in range(1, n):
                t = self.torus.shifted(axis, by)
                self._copy(c, site, send_ref(c, t), rx(c).at[by - 1], axis, by)

        def finish(c):
            self._arrived(c, site, rx(c))

            def add(r0, size):
                value = own(c, r0, size)
                for i in range(n - 1):
                    value = value + rx(c)[i, pl.ds(r0, size), :].astype(F32)
                total(c, r0, size, value)

            rows_loop(rows, lanes, add)
            self._left(c, rx(c))

        return [Step(start, finish)]

    def _direct_gather(self, axis, mine, like):
        n = DIMS[axis]
        site = self._site()

        def start(c):
            for by in range(1, n):
                self._copy(c, site, mine(c), mine(c), axis, by)

        def finish(c):
            self._arrived(c, site, like(c))
            self._left(c, like(c))

        return [Step(start, finish)]

    def _steps(self):
        a1, a2, a3 = self.order
        rows1, lanes2, rows3 = self.rows1, self.lanes2, self.rows3
        at = [self.torus.at[a] for a in self.order]
        chunk = self.chunk

        def block1(c, t, r0, n):
            return chunk(c).at[ds(t * rows1 + r0, n, 16), :]

        def own1(c, t, r0, n):
            return chunk(c)[ds(t * rows1 + r0, n, 16), :].astype(F32)

        def total1(c, r0, n, value):
            at_ = ds(r0, n, 16)
            self.p32[at_, :] = value
            self.pb[at_, :] = value.astype(BF16)

        steps = self._chain(a1, rows1, self.far, BLOCK, block1, own1, self._blocks(self.rx1), total1)

        def own2(c, t, r0, n):
            return self.p32[ds(r0, n, 16), ds(t * lanes2, lanes2)]

        def total2(c, r0, n, value):
            at_ = ds(r0, n, 16)
            self.r32[at_, :] = value
            self.rb[at_, :] = value.astype(BF16)

        if self.chained:
            steps += self._chain(
                a2,
                rows1,
                rows1 // 2,
                lanes2,
                lambda c, t, r0, n: self.pb.at[ds(r0, n, 16), ds(t * lanes2, lanes2)],
                own2,
                self._blocks(self.rx2),
                total2,
            )
        else:
            steps += self._direct(
                a2,
                rows1,
                lanes2,
                lambda c, t: self.pb.at[:, ds(t * lanes2, lanes2)],
                lambda c, r0, n: own2(c, at[1], r0, n),
                lambda c: self.rx2.at[lax.rem(c, SLOTS)],
                total2,
            )

        def final(c):
            return chunk(c).at[ds(at[0] * rows1 + at[2] * rows3, rows3, 16), ds(at[1] * lanes2, lanes2)]

        def total3(c, r0, n, value):
            final(c)[ds(r0, n, 16), :] = value.astype(BF16)

        steps += self._direct(
            a3,
            rows3,
            lanes2,
            lambda c, t: self.rb.at[ds(t * rows3, rows3, 16), :],
            lambda c, r0, n: self.r32[ds(at[2] * rows3 + r0, n, 16), :],
            lambda c: self.rx3.at[lax.rem(c, SLOTS)],
            total3,
        )
        steps += self._direct_gather(a3, final, lambda c: self.rx3.at[lax.rem(c, SLOTS)])

        def block2(c, t, r0, n):
            return chunk(c).at[ds(at[0] * rows1 + r0, n, 16), ds(t * lanes2, lanes2)]

        if self.chained:
            steps += self._chain_gather(a2, rows1, rows1 // 2, block2, lambda c, n: chunk(c).at[pl.ds(0, rows1), pl.ds(0, n * lanes2)])
        else:
            steps += self._direct_gather(a2, lambda c: block2(c, at[1], 0, rows1), lambda c: self.rx2.at[lax.rem(c, SLOTS)])
        steps += self._chain_gather(a1, rows1, self.far, block1, lambda c, n: chunk(c).at[pl.ds(0, n * rows1), :])
        return steps

    @staticmethod
    def scratch(order, chained, chunks):
        n1, n2, n3 = (DIMS[a] for a in order)
        rows1, lanes2 = BLOCK // n1, BLOCK // n2
        rx2 = (chunks, n2 - 1, rows1, lanes2) if chained else (chunks, n2 - 1, rows1, lanes2)
        return [
            pltpu.VMEM((chunks, n1 - 1, rows1, BLOCK), BF16),
            pltpu.VMEM(rx2, BF16),
            pltpu.VMEM((chunks, n3 - 1, rows1 // n3, lanes2), BF16),
            pltpu.VMEM((rows1, BLOCK), F32),
            pltpu.VMEM((rows1, BLOCK), BF16),
            pltpu.VMEM((rows1, lanes2), F32),
            pltpu.VMEM((rows1, lanes2), BF16),
        ]

    @staticmethod
    def n_sites(order, chained):
        k1, k2 = DIMS[order[0]] // 2, DIMS[order[1]] // 2
        return 2 * k1 + (2 * k2 if chained else 2) + 2


DOWN, GATE, UP = range(3)
COLOURS = (((0, 1, 2), True, 0.375), ((1, 0, 2), True, 0.5), ((2, 0, 1), False, 0.25))


def dot(a, b, dims=(((1,), (0,)), ((), ()))):
    return lax.dot_general(a, b, dims, preferred_element_type=F32)


def inverse_rms(wide):
    return lax.rsqrt(jnp.mean(wide * wide, -1, keepdims=True) + 1e-6)


def normed(h):
    wide = h.astype(F32)
    return (wide * inverse_rms(wide)).astype(BF16)


def sigmoid(x):
    return 0.5 * jnp.tanh(0.5 * x) + 0.5


class Compute:
    def __init__(self, weights, dh, h, a, wide):
        self.weights = weights
        self.dh = dh
        self.h = h
        self.a = a
        self.wide = wide
        self.size = a.shape[0] // 4

    def _quarters(self, what, first, count):
        value = self.wide[4 * what + first : 4 * what + first + count, pl.ds(0, self.size), :]
        return value.reshape(count * self.size, BLOCK).astype(BF16)

    def forward(self, wait, then):
        blocks, size = self.weights.shape[2], self.size

        def tile(i, at, wait):
            h = self.dh[at, :]
            a = normed(h)
            for block in range(blocks):
                wait("in", block)
                for first in range(0, BLOCK, BLOCK // 2):
                    part = pl.ds(first, BLOCK // 2)
                    gate = dot(a, self.weights[GATE, 0, block, :, part])
                    up = dot(a, self.weights[UP, 0, block, :, part])
                    self.wide[4 * block + i, pl.ds(0, size), part] = gate * sigmoid(gate) * up
            wait("out", 0)
            out = None
            for block in range(blocks):
                act = self.wide[4 * block + i, pl.ds(0, size), :].astype(BF16)
                more = dot(act, self.weights[DOWN, 0, block])
                out = more if out is None else out + more
            h = h + out.astype(BF16)
            self.h[at, :] = h
            self.a[at, :] = normed(h)
            then(at)

        wait("x", 0)
        tile(0, pl.ds(0, size), wait)
        wait("x", 1)

        def one(i, _):
            tile(i, pl.ds(pl.multiple_of(i * size, size), size), lambda what, i: None)
            return 0

        lax.fori_loop(1, 4, one, 0)

    def back(self, number, block, tile):
        at, rows = pl.ds(tile * self.size, self.size), pl.ds(0, self.size)
        for first in range(0, BLOCK, BLOCK // 2):
            part = pl.ds(first, BLOCK // 2)
            a = self.a[at, :]
            gate = dot(a, self.weights[GATE, number, block, :, part])
            up = dot(a, self.weights[UP, number, block, :, part])
            by = dot(self.dh[at, :], self.weights[DOWN, number, block, part, :], NT).astype(BF16).astype(F32)
            s = sigmoid(gate)
            silu = gate * s
            self.wide[4 * DOWN + tile, rows, part] = silu * up
            self.wide[4 * GATE + tile, rows, part] = by * up * (s + silu * (1.0 - s))
            self.wide[4 * UP + tile, rows, part] = by * silu

    def gradient(self, which, into):
        by = self._quarters(which, 0, 4)
        into[...] = (dot(by, self.dh[...], TN) if which == DOWN else dot(self.a[...], by, TN)).astype(BF16)

    def inputs(self, block, tile):
        part = dot(self._quarters(GATE, 2 * tile, 2), self.weights[GATE, 1, block], NT)
        part = part + dot(self._quarters(UP, 2 * tile, 2), self.weights[UP, 1, block], NT)
        at = pl.ds(12 + 2 * tile, 2), pl.ds(0, self.size)
        self.wide[at] = jnp.where(block == 0, 0.0, self.wide[at]) + part.reshape(2, self.size, BLOCK)

    def below(self, tile):
        block, size = self.weights.shape[2] - 1, self.size // 2

        def one(i, _):
            at = pl.ds(pl.multiple_of(i * size, size), size)
            quarter, rows = lax.div(i, 2), pl.ds(pl.multiple_of(lax.rem(i, 2) * size, size), size)
            by = self.wide[12 + quarter, rows, :]
            for which in (GATE, UP):
                by = by + dot(self.wide[4 * which + quarter, rows, :].astype(BF16), self.weights[which, 1, block], NT)
            by = by.astype(BF16).astype(F32)
            wide = self.h[at, :].astype(F32)
            scale = inverse_rms(wide)
            by = by * scale - wide * (scale * scale * scale * jnp.mean(by * wide, -1, keepdims=True))
            self.dh[at, :] = self.dh[at, :] + by.astype(BF16)
            self.a[at, :] = normed(self.a[at, :])
            return 0

        lax.fori_loop(4 * tile, 4 * tile + 4, one, 0)


def moment_blocks(layers, blocks):
    order = [(number, k, which, j) for number in reversed(range(layers)) for which in range(3) for j in range(blocks) for k in range(2)]
    places = {}
    for i, key in enumerate(order):
        if i < KEPT:
            places[key] = 0, i
        elif i < KEPT + 16:
            places[key] = 1, i - KEPT
        else:
            places[key] = 2, i - KEPT - 16
    return places


def block_at(arrays, which, number, j, r0=0, n=BLOCK):
    if which == DOWN:
        return arrays[2].at[number, ds(j * BLOCK + r0, n), :]
    return arrays[which - 1].at[number, ds(r0, n), ds(j * BLOCK, BLOCK)]


def train_kernel(x, dy, *refs):
    weights, moments, (g, w, kept, wide), refs = refs[:3], (refs[3:6], refs[6:9]), refs[9:13], refs[13:]
    (dh, h, a), scratch = refs[:3], refs[3:]
    scratch, (send_sems, recv_sems, in_sems) = scratch[:-3], scratch[-3:]
    _, layers, blocks, _, _ = w.shape
    chunks = layers * blocks
    assert layers == 2
    torus = Torus()
    wait_barrier = torus.barrier()
    size = dh.shape[0] // 4

    def weight(which, number, j):
        return block_at(weights, which, number, j), w.at[which, number, j]

    first = x.at[0, pl.ds(0, size)], dh.at[pl.ds(0, size)]
    rest = x.at[0, pl.ds(size, 3 * size)], dh.at[pl.ds(size, 3 * size)]
    groups = {("x", 0): ([first], first[1])}
    for j in range(blocks):
        groups["in", j] = [weight(which, 0, j) for which in (GATE, UP)], w.at[pl.ds(GATE, 2), 0, j]
        if j == 0:
            groups["out", 0] = [weight(DOWN, 0, i) for i in range(blocks)], w.at[DOWN, 0]
    groups["x", 1] = [rest], rest[1]
    groups["late", 0] = [weight(which, 1, j) for j in range(blocks) for which in range(3)], w.at[:, 1]
    groups["again", 0] = [(x.at[0], a)], a
    places = moment_blocks(layers, blocks)
    for n, into in enumerate((kept, wide)):
        pairs = [(block_at(moments[k], i, number, j), into.at[p]) for (number, k, i, j), (m, p) in places.items() if m == n]
        groups["moments", n] = pairs, into.at[pl.ds(0, len(pairs))]
    sem_of = {key: i for i, key in enumerate(groups)}
    dy_sem = in_sems.at[len(groups)]

    def begin(*key):
        for src, dst in groups[key][0]:
            pltpu.make_async_copy(src, dst, in_sems.at[sem_of[key]]).start()

    def wait(*key):
        like = groups[key][1]
        pltpu.make_async_copy(like, like, in_sems.at[sem_of[key]]).wait()

    for key in groups:
        if key[0] not in ("again", "moments"):
            begin(*key)
    compute = Compute(w, dh, h, a, wide)
    compute.forward(wait, lambda at: pltpu.make_async_copy(dy.at[0, at, :], dh.at[at, :], dy_sem).start())
    wait("late", 0)
    pltpu.make_async_copy(dh, dh, dy_sem).wait()
    begin("moments", 0)
    wait_barrier()

    sites, exchanges = [0], []
    for k, (order, chained, far) in enumerate(COLOURS):
        rx, temporary = scratch[7 * k : 7 * k + 3], scratch[7 * k + 3 : 7 * k + 7]
        sems = send_sems.at[k], recv_sems
        exchanges.append(Exchange(torus, order, chained, far, lambda c, k=k: g.at[c, k], rx, *temporary, sems, sites))

    def stage(c, k, s):
        steps = exchanges[k].steps
        if s:
            steps[s - 1].finish(c)
        if s < len(steps):
            steps[s].start(c)

    def work(name, c):
        number, block = layers - 1 - lax.div(c, blocks), lax.rem(c, blocks)
        what, _, tile = name.partition(" ")
        if what == "inputs":

            @pl.when(c < blocks - 1)
            def _():
                compute.inputs(block, int(tile))

            @pl.when(c == blocks - 1)
            def _():
                if tile == "0":
                    wait("again", 0)
                compute.below(int(tile))

            return
        if what == LAST:
            @pl.when(c == blocks - 1)
            def _():
                begin("again", 0)

        @pl.when(c < chunks)
        def _():
            if what == "back":
                compute.back(number, block, int(tile))
            else:
                which = ("down", "gate", "up").index(what)
                compute.gradient(which, g.at[c, which])

        if what == LAST:
            @pl.when(c == chunks - 1)
            def _():
                begin("moments", 1)

    lags = [item[2] for item in PERIOD if not isinstance(item, str)]

    def body(period, _):
        i = 0
        while i < len(PERIOD):
            if isinstance(PERIOD[i], str):
                work(PERIOD[i], period)
                i += 1
                continue
            j = i
            while j < len(PERIOD) and not isinstance(PERIOD[j], str) and PERIOD[j][2] == PERIOD[i][2]:
                j += 1
            c = period - PERIOD[i][2]

            @pl.when((c >= 0) & (c < chunks))
            def _(c=c, group=PERIOD[i:j]):
                for k, s, _ in group:
                    stage(c, k, s)

            i = j
        return 0

    lax.fori_loop(0, chunks + max(lags), body, 0)
    wait("moments", 0)
    wait("moments", 1)


def gradients(x, dy, weights, moments):
    gate, up, down = weights
    layers, d, ff = gate.shape
    tokens = x.shape[1]
    chunks = layers * ff // BLOCK
    scratch = [pltpu.VMEM((tokens, d), BF16) for _ in range(3)]
    n_sites = 0
    for order, chained, _ in COLOURS:
        scratch += Exchange.scratch(order, chained, SLOTS)
        n_sites += Exchange.n_sites(order, chained)
    scratch += [pltpu.SemaphoreType.DMA((len(COLOURS), chunks)), pltpu.SemaphoreType.DMA((SLOTS, n_sites)), pltpu.SemaphoreType.DMA((12,))]
    out = [
        pltpu.VMEM((chunks, 3, BLOCK, BLOCK), BF16),
        pltpu.VMEM((3, layers, ff // BLOCK, BLOCK, BLOCK), BF16),
        pltpu.VMEM((KEPT, BLOCK, BLOCK), F32),
        pltpu.VMEM((16, BLOCK, BLOCK), F32),
    ]
    return pl.pallas_call(
        train_kernel,
        out_shape=out,
        in_specs=[pl.BlockSpec(memory_space=pltpu.HBM)] * 11,
        out_specs=[pl.BlockSpec(memory_space=pltpu.VMEM)] * len(out),
        scratch_shapes=scratch,
        compiler_params=pltpu.CompilerParams(collective_id=0, has_side_effects=True, vmem_limit_bytes=VMEM_LIMIT),
        name="gradients",
    )(x, dy, *weights, *moments)


def adamw(w, m, v, g):
    m = 0.9 * m + 0.1 * g
    v = 0.95 * v + 0.05 * g * g
    step = m * lax.rsqrt(v + 1e-8) + 0.1 * w
    return (w - 0.02 * step).astype(BF16), m, v


def adamw_kernel(g, w, kept, wide, *refs):
    moments, new, refs = (refs[:3], refs[3:6]), (refs[6:9], refs[9:12], refs[12:15]), refs[15:]
    own, *staged, in_sems, out_sems = refs
    _, layers, blocks, _, _ = w.shape
    parts = BLOCK // PIECE
    places = moment_blocks(layers, blocks)

    def load(key):
        number, k, which, j = key
        p = places[key][1]
        return pltpu.make_async_copy(block_at(moments[k], which, number, j), own.at[p], in_sems.at[p])

    def save(slot, which, number, j, r0):
        return [
            pltpu.make_async_copy(staged[k].at[slot], block_at(new[k], which, number, j, r0, PIECE), out_sems.at[slot, k])
            for k in range(3)
        ]

    for key, (where, _) in places.items():
        if where == 2:
            load(key).start()

    done = 0
    for number, _, which, j in [key for key in places if key[1] == 0]:
        here = [places[number, k, which, j] for k in range(2)]
        for k in range(2):
            if here[k][0] == 2:
                load((number, k, which, j)).wait()

        def one(r, _, done=done, number=number, which=which, j=j, here=here):
            n = done + r
            slot = lax.rem(n, OUTPUTS)

            @pl.when(n >= OUTPUTS)
            def _():
                for copy in save(slot, which, number, j, r * PIECE):
                    copy.wait()

            for r0 in range(0, PIECE, STRIP):
                rows = ds(r * PIECE + r0, STRIP)
                grad = g[(layers - 1 - number) * blocks + j, which, rows, :].astype(F32)
                m, v = ((kept, wide, own)[where][p, rows, :] for where, p in here)
                now = adamw(w[which, number, j, rows, :].astype(F32), m, v, grad)
                for k in range(3):
                    staged[k][slot, pl.ds(r0, STRIP), :] = now[k]
            for copy in save(slot, which, number, j, r * PIECE):
                copy.start()
            return 0

        lax.fori_loop(0, parts, one, 0)
        done += parts
    for slot in range(OUTPUTS):
        for copy in save(slot, DOWN, 0, 0, 0):
            copy.wait()


def update(g, w, kept, wide, weights, moments):
    _, layers, blocks, _, _ = w.shape
    vmem, hbm = pl.BlockSpec(memory_space=pltpu.VMEM), pl.BlockSpec(memory_space=pltpu.HBM)
    own = max(1, sum(where == 2 for where, _ in moment_blocks(layers, blocks).values()))
    return pl.pallas_call(
        adamw_kernel,
        out_shape=[jax.ShapeDtypeStruct(a.shape, BF16) for a in weights] + [jax.ShapeDtypeStruct(a.shape, F32) for a in moments],
        in_specs=[vmem] * 4 + [hbm] * 6,
        out_specs=[hbm] * 9,
        scratch_shapes=[
            pltpu.VMEM((own, BLOCK, BLOCK), F32),
            *(pltpu.VMEM((OUTPUTS, PIECE, BLOCK), dtype) for dtype in (BF16, F32, F32)),
            pltpu.SemaphoreType.DMA((own,)),
            pltpu.SemaphoreType.DMA((OUTPUTS, 3)),
        ],
        compiler_params=pltpu.CompilerParams(vmem_limit_bytes=UPDATE_LIMIT),
        name="update",
    )(g, w, kept, wide, *moments)


def solution(mesh):
    def step(x, dy, *arrays):
        weights, moments = arrays[:3], arrays[3:]
        there = gradients(x, dy, weights, moments)
        there = [pltpu.with_memory_space_constraint(a, pltpu.VMEM) for a in there]
        moments = [pltpu.with_memory_space_constraint(a, pltpu.HBM) for a in moments]
        return tuple(update(*there, weights, moments))

    return jax.shard_map(
        step,
        mesh=mesh,
        in_specs=(P(("rep", "dp"), None, None),) * 2 + (P(None, None, None),) * 9,
        out_specs=(P("rep", None, None),) * 9,
        check_vma=False,
    )
```

```python
import functools

import jax
import jax.numpy as jnp
from jax import lax
from jax.experimental import pallas as pl
from jax.experimental.pallas import tpu as pltpu
from jax.sharding import PartitionSpec as P

MESH = pl.DeviceIdType.MESH
DIMS = (4, 4, 8)
BLOCK = 512
HEAD_START_NS = 2098
LAST = "down"
KEPT = 14
PIECE = 128
STRIP = 32
SLOTS = 3
OUTPUTS = 8
PERIOD = (
    "back 0",
    (2, 7, 3), (0, 9, 5),
    "back 1",
    (1, 4, 2), (1, 1, 1), (2, 2, 1),
    "back 2",
    (0, 4, 2), (1, 6, 3), (2, 5, 2), (0, 1, 1), (0, 8, 4), (2, 11, 5),
    "back 3",
    (0, 6, 3), (2, 8, 3), (1, 8, 4),
    "up",
    (2, 0, 0), (2, 3, 1), (1, 2, 1),
    "gate",
    (2, 6, 2), (0, 2, 1),
    "down",
    (1, 5, 2), (0, 10, 5), (1, 0, 0), (0, 5, 2),
    "inputs 0",
    (2, 10, 4), (0, 7, 3), (1, 3, 1), (2, 1, 0), (1, 10, 5), (0, 0, 0), (2, 4, 1), (1, 7, 3), (2, 12, 5), (2, 9, 3),
    "inputs 1",
    (0, 3, 1), (1, 9, 4),
)
VMEM_LIMIT = UPDATE_LIMIT = 16_700_000
TN = (((0,), (0,)), ((), ()))
NT = (((1,), (1,)), ((), ()))
BF16, F32 = jnp.bfloat16, jnp.float32


def ds(start, size, multiple=None):
    if isinstance(start, int):
        return pl.ds(start, size)
    return pl.ds(pl.multiple_of(start, multiple or size), size)


class Torus:
    def __init__(self):
        i = lax.axis_index("dp")
        nx, ny, nz = DIMS
        self.at = (lax.div(i, ny * nz), lax.rem(lax.div(i, nz), ny), lax.rem(i, nz))
        self._places, self._devices = {}, {}
        for axis, n in enumerate(DIMS):
            for by in range(n):
                self._places[axis, by] = place = lax.rem(self.at[axis] + by, n) if by else self.at[axis]
                to = list(self.at)
                to[axis] = place
                self._devices[axis, by] = (to[0] * ny + to[1]) * nz + to[2]

    def shifted(self, axis, by):
        return self._places[axis, by % DIMS[axis]]

    def device(self, axis, by):
        return {"dp": self._devices[axis, by % DIMS[axis]]}

    def barrier(self):
        sem = pltpu.get_barrier_semaphore()
        peers = [(axis, by) for axis in range(3) for by in range(1, DIMS[axis])]
        for axis, by in peers:
            pl.semaphore_signal(sem, inc=1, device_id=self.device(axis, by), device_id_type=MESH)
        return lambda: pl.semaphore_wait(sem, len(peers))


class Step:
    def __init__(self, start, finish):
        self.start, self.finish = start, finish


def rows_loop(rows, lanes, body):
    size = min(rows, 32 * 1024 // lanes)
    for r0 in range(0, rows, size):
        body(r0, min(size, rows - r0))


class Exchange:
    def __init__(self, torus, order, chained, far, chunk, rx, p32, pb, r32, rb, sems, sites):
        self.torus, self.order, self.chained = torus, order, chained
        self.chunk = chunk
        self.rx1, self.rx2, self.rx3 = rx
        self.p32, self.pb, self.r32, self.rb = p32, pb, r32, rb
        self.send_sems, self.recv_sems = sems
        self.sites = sites
        n1, n2, n3 = (DIMS[a] for a in order)
        self.rows1 = BLOCK // n1
        self.far = int(self.rows1 * far) // 16 * 16
        self.lanes2 = BLOCK // n2
        self.rows3 = self.rows1 // n3
        self.steps = self._steps()

    def _site(self):
        s = self.sites[0]
        self.sites[0] += 1
        return s

    def _copy(self, c, site, src, dst, axis, by):
        pltpu.make_async_remote_copy(
            src_ref=src,
            dst_ref=dst,
            send_sem=self.send_sems.at[c],
            recv_sem=self.recv_sems.at[lax.rem(c, SLOTS), site],
            device_id=self.torus.device(axis, by),
            device_id_type=MESH,
        ).start()

    @staticmethod
    def _blocks(ref):
        def rx(c, i, n=None):
            return ref.at[lax.rem(c, SLOTS), i if n is None else pl.ds(i, n)]

        return rx

    def _arrived(self, c, site, like):
        pltpu.make_async_copy(like, like, self.recv_sems.at[lax.rem(c, SLOTS), site]).wait()

    def _left(self, c, like):
        pltpu.make_async_copy(like, like, self.send_sems.at[c]).wait()

    def _chain(self, axis, rows, far, lanes, send_ref, own, rx, total):
        k = DIMS[axis] // 2
        ways = ((1, 0, (0, far), (far, rows - far)), (-1, 1, (far, rows - far), (0, far)))

        def got(c, s, w):
            return rx(c, 0 if s == 1 else 2 * s - 3 + w)

        steps = []
        for s in range(1, k + 1):
            site = self._site()

            def start(c, s=s, site=site):
                for way, w, mine, others in ways:
                    t = self.torus.shifted(axis, way * (k + 1 - s))
                    dst = got(c, s, w)
                    if s == 1:
                        self._copy(c, site, send_ref(c, t, *mine), dst.at[ds(*mine, 16), :], axis, way)
                    elif s == 2:
                        self._copy(c, site, got(c, 1, w).at[ds(*mine, 16), :], dst.at[ds(*mine, 16), :], axis, way)
                        self._copy(c, site, send_ref(c, t, *others), dst.at[ds(*others, 16), :], axis, way)
                    else:
                        self._copy(c, site, got(c, s - 1, w), dst, axis, way)

            def finish(c, s=s, site=site):
                like = rx(c, 0) if s == 1 else rx(c, 2 * s - 3, 2)
                self._arrived(c, site, like)
                if s < k:
                    for way, w, mine, _ in ways:
                        t = self.torus.shifted(axis, way * (k - s))
                        first, count = mine if s == 1 else (0, rows)
                        here = got(c, s, w)

                        def add(r0, size, here=here, t=t, first=first):
                            at = pl.ds(first + r0, size)
                            here[at, :] = (here[at, :].astype(F32) + own(c, t, first + r0, size)).astype(BF16)

                        rows_loop(count, lanes, add)
                else:
                    me = self.torus.shifted(axis, 0)
                    for _, here, (first, count), _ in ways:

                        def add(r0, size, here=here, first=first):
                            at = pl.ds(first + r0, size)
                            value = own(c, me, first + r0, size)
                            for w in range(2):
                                if k > 1 or w == here:
                                    value = value + got(c, s, w)[at, :].astype(F32)
                            total(c, first + r0, size, value)

                        rows_loop(count, lanes, add)
                self._left(c, like)

            steps.append(Step(start, finish))
        return steps

    def _chain_gather(self, axis, rows, far, block, like):
        k = DIMS[axis] // 2
        ways = ((1, (0, far)), (-1, (far, rows - far)))
        steps = []
        for s in range(1, k + 1):
            site = self._site()

            def start(c, s=s, site=site):
                for way, mine in ways:
                    t = self.torus.shifted(axis, -way * (s - 1))
                    ref = block(c, t, *mine) if s == k else block(c, t, 0, rows)
                    self._copy(c, site, ref, ref, axis, way)

            def finish(c, s=s, site=site):
                both = like(c, 1 if s == k else 2)
                self._arrived(c, site, both)
                self._left(c, both)

            steps.append(Step(start, finish))
        return steps

    def _direct(self, axis, rows, lanes, send_ref, own, rx, total):
        n = DIMS[axis]
        site = self._site()

        def start(c):
            for by in range(1, n):
                t = self.torus.shifted(axis, by)
                self._copy(c, site, send_ref(c, t), rx(c).at[by - 1], axis, by)

        def finish(c):
            self._arrived(c, site, rx(c))

            def add(r0, size):
                value = own(c, r0, size)
                for i in range(n - 1):
                    value = value + rx(c)[i, pl.ds(r0, size), :].astype(F32)
                total(c, r0, size, value)

            rows_loop(rows, lanes, add)
            self._left(c, rx(c))

        return [Step(start, finish)]

    def _direct_gather(self, axis, mine, like):
        n = DIMS[axis]
        site = self._site()

        def start(c):
            for by in range(1, n):
                self._copy(c, site, mine(c), mine(c), axis, by)

        def finish(c):
            self._arrived(c, site, like(c))
            self._left(c, like(c))

        return [Step(start, finish)]

    def _steps(self):
        a1, a2, a3 = self.order
        rows1, lanes2, rows3 = self.rows1, self.lanes2, self.rows3
        at = [self.torus.at[a] for a in self.order]
        chunk = self.chunk

        def block1(c, t, r0, n):
            return chunk(c).at[ds(t * rows1 + r0, n, 16), :]

        def own1(c, t, r0, n):
            return chunk(c)[ds(t * rows1 + r0, n, 16), :].astype(F32)

        def total1(c, r0, n, value):
            at_ = ds(r0, n, 16)
            self.p32[at_, :] = value
            self.pb[at_, :] = value.astype(BF16)

        steps = self._chain(a1, rows1, self.far, BLOCK, block1, own1, self._blocks(self.rx1), total1)

        def own2(c, t, r0, n):
            return self.p32[ds(r0, n, 16), ds(t * lanes2, lanes2)]

        def total2(c, r0, n, value):
            at_ = ds(r0, n, 16)
            self.r32[at_, :] = value
            self.rb[at_, :] = value.astype(BF16)

        if self.chained:
            steps += self._chain(
                a2,
                rows1,
                rows1 // 2,
                lanes2,
                lambda c, t, r0, n: self.pb.at[ds(r0, n, 16), ds(t * lanes2, lanes2)],
                own2,
                self._blocks(self.rx2),
                total2,
            )
        else:
            steps += self._direct(
                a2,
                rows1,
                lanes2,
                lambda c, t: self.pb.at[:, ds(t * lanes2, lanes2)],
                lambda c, r0, n: own2(c, at[1], r0, n),
                lambda c: self.rx2.at[lax.rem(c, SLOTS)],
                total2,
            )

        def final(c):
            return chunk(c).at[ds(at[0] * rows1 + at[2] * rows3, rows3, 16), ds(at[1] * lanes2, lanes2)]

        def total3(c, r0, n, value):
            final(c)[ds(r0, n, 16), :] = value.astype(BF16)

        steps += self._direct(
            a3,
            rows3,
            lanes2,
            lambda c, t: self.rb.at[ds(t * rows3, rows3, 16), :],
            lambda c, r0, n: self.r32[ds(at[2] * rows3 + r0, n, 16), :],
            lambda c: self.rx3.at[lax.rem(c, SLOTS)],
            total3,
        )
        steps += self._direct_gather(a3, final, lambda c: self.rx3.at[lax.rem(c, SLOTS)])

        def block2(c, t, r0, n):
            return chunk(c).at[ds(at[0] * rows1 + r0, n, 16), ds(t * lanes2, lanes2)]

        if self.chained:
            steps += self._chain_gather(a2, rows1, rows1 // 2, block2, lambda c, n: chunk(c).at[pl.ds(0, rows1), pl.ds(0, n * lanes2)])
        else:
            steps += self._direct_gather(a2, lambda c: block2(c, at[1], 0, rows1), lambda c: self.rx2.at[lax.rem(c, SLOTS)])
        steps += self._chain_gather(a1, rows1, self.far, block1, lambda c, n: chunk(c).at[pl.ds(0, n * rows1), :])
        return steps

    @staticmethod
    def scratch(order, chained, chunks):
        n1, n2, n3 = (DIMS[a] for a in order)
        rows1, lanes2 = BLOCK // n1, BLOCK // n2
        rx2 = (chunks, n2 - 1, rows1, lanes2) if chained else (chunks, n2 - 1, rows1, lanes2)
        return [
            pltpu.VMEM((chunks, n1 - 1, rows1, BLOCK), BF16),
            pltpu.VMEM(rx2, BF16),
            pltpu.VMEM((chunks, n3 - 1, rows1 // n3, lanes2), BF16),
            pltpu.VMEM((rows1, BLOCK), F32),
            pltpu.VMEM((rows1, BLOCK), BF16),
            pltpu.VMEM((rows1, lanes2), F32),
            pltpu.VMEM((rows1, lanes2), BF16),
        ]

    @staticmethod
    def n_sites(order, chained):
        k1, k2 = DIMS[order[0]] // 2, DIMS[order[1]] // 2
        return 2 * k1 + (2 * k2 if chained else 2) + 2


DOWN, GATE, UP = range(3)
COLOURS = (((0, 1, 2), True, 0.375), ((1, 0, 2), True, 0.5), ((2, 0, 1), False, 0.25))


def dot(a, b, dims=(((1,), (0,)), ((), ()))):
    return lax.dot_general(a, b, dims, preferred_element_type=F32)


def inverse_rms(wide):
    return lax.rsqrt(jnp.mean(wide * wide, -1, keepdims=True) + 1e-6)


def normed(h):
    wide = h.astype(F32)
    return (wide * inverse_rms(wide)).astype(BF16)


def sigmoid(x):
    return 0.5 * jnp.tanh(0.5 * x) + 0.5


class Compute:
    def __init__(self, weights, dh, h, a, wide):
        self.weights = weights
        self.dh = dh
        self.h = h
        self.a = a
        self.wide = wide
        self.size = a.shape[0] // 4

    def _quarters(self, what, first, count):
        value = self.wide[4 * what + first : 4 * what + first + count, pl.ds(0, self.size), :]
        return value.reshape(count * self.size, BLOCK).astype(BF16)

    def forward(self, wait, then):
        blocks, size = self.weights.shape[2], self.size

        def tile(i, at, wait):
            h = self.dh[at, :]
            a = normed(h)
            for block in range(blocks):
                wait("in", block)
                for first in range(0, BLOCK, BLOCK // 2):
                    part = pl.ds(first, BLOCK // 2)
                    gate = dot(a, self.weights[GATE, 0, block, :, part])
                    up = dot(a, self.weights[UP, 0, block, :, part])
                    self.wide[4 * block + i, pl.ds(0, size), part] = gate * sigmoid(gate) * up
            wait("out", 0)
            out = None
            for block in range(blocks):
                act = self.wide[4 * block + i, pl.ds(0, size), :].astype(BF16)
                more = dot(act, self.weights[DOWN, 0, block])
                out = more if out is None else out + more
            h = h + out.astype(BF16)
            self.h[at, :] = h
            self.a[at, :] = normed(h)
            then(at)

        wait("x", 0)
        tile(0, pl.ds(0, size), wait)
        wait("x", 1)

        def one(i, _):
            tile(i, pl.ds(pl.multiple_of(i * size, size), size), lambda what, i: None)
            return 0

        lax.fori_loop(1, 4, one, 0)

    def back(self, number, block, tile):
        at, rows = pl.ds(tile * self.size, self.size), pl.ds(0, self.size)
        for first in range(0, BLOCK, BLOCK // 2):
            part = pl.ds(first, BLOCK // 2)
            a = self.a[at, :]
            gate = dot(a, self.weights[GATE, number, block, :, part])
            up = dot(a, self.weights[UP, number, block, :, part])
            by = dot(self.dh[at, :], self.weights[DOWN, number, block, part, :], NT).astype(BF16).astype(F32)
            s = sigmoid(gate)
            silu = gate * s
            self.wide[4 * DOWN + tile, rows, part] = silu * up
            self.wide[4 * GATE + tile, rows, part] = by * up * (s + silu * (1.0 - s))
            self.wide[4 * UP + tile, rows, part] = by * silu

    def gradient(self, which, into):
        by = self._quarters(which, 0, 4)
        into[...] = (dot(by, self.dh[...], TN) if which == DOWN else dot(self.a[...], by, TN)).astype(BF16)

    def inputs(self, block, tile):
        part = dot(self._quarters(GATE, 2 * tile, 2), self.weights[GATE, 1, block], NT)
        part = part + dot(self._quarters(UP, 2 * tile, 2), self.weights[UP, 1, block], NT)
        at = pl.ds(12 + 2 * tile, 2), pl.ds(0, self.size)
        self.wide[at] = jnp.where(block == 0, 0.0, self.wide[at]) + part.reshape(2, self.size, BLOCK)

    def below(self, tile):
        block, size = self.weights.shape[2] - 1, self.size // 2

        def one(i, _):
            at = pl.ds(pl.multiple_of(i * size, size), size)
            quarter, rows = lax.div(i, 2), pl.ds(pl.multiple_of(lax.rem(i, 2) * size, size), size)
            by = self.wide[12 + quarter, rows, :]
            for which in (GATE, UP):
                by = by + dot(self.wide[4 * which + quarter, rows, :].astype(BF16), self.weights[which, 1, block], NT)
            by = by.astype(BF16).astype(F32)
            wide = self.h[at, :].astype(F32)
            scale = inverse_rms(wide)
            by = by * scale - wide * (scale * scale * scale * jnp.mean(by * wide, -1, keepdims=True))
            self.dh[at, :] = self.dh[at, :] + by.astype(BF16)
            self.a[at, :] = normed(self.a[at, :])
            return 0

        lax.fori_loop(4 * tile, 4 * tile + 4, one, 0)


def moment_blocks(layers, blocks):
    order = [(number, k, which, j) for number in reversed(range(layers)) for which in range(3) for j in range(blocks) for k in range(2)]
    places = {}
    for i, key in enumerate(order):
        if i < KEPT:
            places[key] = 0, i
        elif i < KEPT + 16:
            places[key] = 1, i - KEPT
        else:
            places[key] = 2, i - KEPT - 16
    return places


def block_at(arrays, which, number, j, r0=0, n=BLOCK):
    if which == DOWN:
        return arrays[2].at[number, ds(j * BLOCK + r0, n), :]
    return arrays[which - 1].at[number, ds(r0, n), ds(j * BLOCK, BLOCK)]


def train_kernel(x, dy, *refs):
    weights, moments, (g, w, kept, wide), refs = refs[:3], (refs[3:6], refs[6:9]), refs[9:13], refs[13:]
    (dh, h, a), scratch = refs[:3], refs[3:]
    scratch, (send_sems, recv_sems, in_sems) = scratch[:-3], scratch[-3:]
    _, layers, blocks, _, _ = w.shape
    chunks = layers * blocks
    assert layers == 2
    torus = Torus()
    wait_barrier = torus.barrier()
    size = dh.shape[0] // 4

    def weight(which, number, j):
        return block_at(weights, which, number, j), w.at[which, number, j]

    first = x.at[0, pl.ds(0, size)], dh.at[pl.ds(0, size)]
    rest = x.at[0, pl.ds(size, 3 * size)], dh.at[pl.ds(size, 3 * size)]
    groups = {("x", 0): ([first], first[1])}
    for j in range(blocks):
        groups["in", j] = [weight(which, 0, j) for which in (GATE, UP)], w.at[pl.ds(GATE, 2), 0, j]
        if j == 0:
            groups["out", 0] = [weight(DOWN, 0, i) for i in range(blocks)], w.at[DOWN, 0]
    groups["x", 1] = [rest], rest[1]
    groups["late", 0] = [weight(which, 1, j) for j in range(blocks) for which in range(3)], w.at[:, 1]
    groups["again", 0] = [(x.at[0], a)], a
    places = moment_blocks(layers, blocks)
    for n, into in enumerate((kept, wide)):
        pairs = [(block_at(moments[k], i, number, j), into.at[p]) for (number, k, i, j), (m, p) in places.items() if m == n]
        groups["moments", n] = pairs, into.at[pl.ds(0, len(pairs))]
    sem_of = {key: i for i, key in enumerate(groups)}
    dy_sem = in_sems.at[len(groups)]

    def begin(*key):
        for src, dst in groups[key][0]:
            pltpu.make_async_copy(src, dst, in_sems.at[sem_of[key]]).start()

    def wait(*key):
        like = groups[key][1]
        pltpu.make_async_copy(like, like, in_sems.at[sem_of[key]]).wait()

    for key in groups:
        if key[0] not in ("again", "moments"):
            begin(*key)
    compute = Compute(w, dh, h, a, wide)

    @pl.when(lax.axis_index("rep") == 1)
    def _():
        pl.delay(HEAD_START_NS)

    compute.forward(wait, lambda at: pltpu.make_async_copy(dy.at[0, at, :], dh.at[at, :], dy_sem).start())
    wait("late", 0)
    pltpu.make_async_copy(dh, dh, dy_sem).wait()
    begin("moments", 0)
    wait_barrier()

    sites, exchanges = [0], []
    for k, (order, chained, far) in enumerate(COLOURS):
        rx, temporary = scratch[7 * k : 7 * k + 3], scratch[7 * k + 3 : 7 * k + 7]
        sems = send_sems.at[k], recv_sems
        exchanges.append(Exchange(torus, order, chained, far, lambda c, k=k: g.at[c, k], rx, *temporary, sems, sites))

    def stage(c, k, s):
        steps = exchanges[k].steps
        if s:
            steps[s - 1].finish(c)
        if s < len(steps):
            steps[s].start(c)

    def work(name, c):
        number, block = layers - 1 - lax.div(c, blocks), lax.rem(c, blocks)
        what, _, tile = name.partition(" ")
        if what == "inputs":

            @pl.when(c < blocks - 1)
            def _():
                compute.inputs(block, int(tile))

            @pl.when(c == blocks - 1)
            def _():
                if tile == "0":
                    wait("again", 0)
                compute.below(int(tile))

            return
        if what == LAST:
            @pl.when(c == blocks - 1)
            def _():
                begin("again", 0)

        @pl.when(c < chunks)
        def _():
            if what == "back":
                compute.back(number, block, int(tile))
            else:
                which = ("down", "gate", "up").index(what)
                compute.gradient(which, g.at[c, which])

        if what == LAST:
            @pl.when(c == chunks - 1)
            def _():
                begin("moments", 1)

    lags = [item[2] for item in PERIOD if not isinstance(item, str)]

    def body(period, _):
        i = 0
        while i < len(PERIOD):
            if isinstance(PERIOD[i], str):
                work(PERIOD[i], period)
                i += 1
                continue
            j = i
            while j < len(PERIOD) and not isinstance(PERIOD[j], str) and PERIOD[j][2] == PERIOD[i][2]:
                j += 1
            c = period - PERIOD[i][2]

            @pl.when((c >= 0) & (c < chunks))
            def _(c=c, group=PERIOD[i:j]):
                for k, s, _ in group:
                    stage(c, k, s)

            i = j
        return 0

    lax.fori_loop(0, chunks + max(lags), body, 0)
    wait("moments", 0)
    wait("moments", 1)


def gradients(x, dy, weights, moments):
    gate, up, down = weights
    layers, d, ff = gate.shape
    tokens = x.shape[1]
    chunks = layers * ff // BLOCK
    scratch = [pltpu.VMEM((tokens, d), BF16) for _ in range(3)]
    n_sites = 0
    for order, chained, _ in COLOURS:
        scratch += Exchange.scratch(order, chained, SLOTS)
        n_sites += Exchange.n_sites(order, chained)
    scratch += [pltpu.SemaphoreType.DMA((len(COLOURS), chunks)), pltpu.SemaphoreType.DMA((SLOTS, n_sites)), pltpu.SemaphoreType.DMA((12,))]
    out = [
        pltpu.VMEM((chunks, 3, BLOCK, BLOCK), BF16),
        pltpu.VMEM((3, layers, ff // BLOCK, BLOCK, BLOCK), BF16),
        pltpu.VMEM((KEPT, BLOCK, BLOCK), F32),
        pltpu.VMEM((16, BLOCK, BLOCK), F32),
    ]
    return pl.pallas_call(
        train_kernel,
        out_shape=out,
        in_specs=[pl.BlockSpec(memory_space=pltpu.HBM)] * 11,
        out_specs=[pl.BlockSpec(memory_space=pltpu.VMEM)] * len(out),
        scratch_shapes=scratch,
        compiler_params=pltpu.CompilerParams(collective_id=0, has_side_effects=True, vmem_limit_bytes=VMEM_LIMIT),
        name="gradients",
    )(x, dy, *weights, *moments)


def adamw(w, m, v, g):
    m = 0.9 * m + 0.1 * g
    v = 0.95 * v + 0.05 * g * g
    step = m * lax.rsqrt(v + 1e-8) + 0.1 * w
    return (w - 0.02 * step).astype(BF16), m, v


def adamw_kernel(g, w, kept, wide, *refs):
    moments, new, refs = (refs[:3], refs[3:6]), (refs[6:9], refs[9:12], refs[12:15]), refs[15:]
    own, *staged, in_sems, out_sems = refs
    _, layers, blocks, _, _ = w.shape
    parts = BLOCK // PIECE
    places = moment_blocks(layers, blocks)

    def load(key):
        number, k, which, j = key
        p = places[key][1]
        return pltpu.make_async_copy(block_at(moments[k], which, number, j), own.at[p], in_sems.at[p])

    def save(slot, which, number, j, r0):
        return [
            pltpu.make_async_copy(staged[k].at[slot], block_at(new[k], which, number, j, r0, PIECE), out_sems.at[slot, k])
            for k in range(3)
        ]

    for key, (where, _) in places.items():
        if where == 2:
            load(key).start()

    done = 0
    for number, _, which, j in [key for key in places if key[1] == 0]:
        here = [places[number, k, which, j] for k in range(2)]
        for k in range(2):
            if here[k][0] == 2:
                load((number, k, which, j)).wait()

        def one(r, _, done=done, number=number, which=which, j=j, here=here):
            n = done + r
            slot = lax.rem(n, OUTPUTS)

            @pl.when(n >= OUTPUTS)
            def _():
                for copy in save(slot, which, number, j, r * PIECE):
                    copy.wait()

            for r0 in range(0, PIECE, STRIP):
                rows = ds(r * PIECE + r0, STRIP)
                grad = g[(layers - 1 - number) * blocks + j, which, rows, :].astype(F32)
                m, v = ((kept, wide, own)[where][p, rows, :] for where, p in here)
                now = adamw(w[which, number, j, rows, :].astype(F32), m, v, grad)
                for k in range(3):
                    staged[k][slot, pl.ds(r0, STRIP), :] = now[k]
            for copy in save(slot, which, number, j, r * PIECE):
                copy.start()
            return 0

        lax.fori_loop(0, parts, one, 0)
        done += parts
    for slot in range(OUTPUTS):
        for copy in save(slot, DOWN, 0, 0, 0):
            copy.wait()


def update(g, w, kept, wide, weights, moments):
    _, layers, blocks, _, _ = w.shape
    vmem, hbm = pl.BlockSpec(memory_space=pltpu.VMEM), pl.BlockSpec(memory_space=pltpu.HBM)
    own = max(1, sum(where == 2 for where, _ in moment_blocks(layers, blocks).values()))
    return pl.pallas_call(
        adamw_kernel,
        out_shape=[jax.ShapeDtypeStruct(a.shape, BF16) for a in weights] + [jax.ShapeDtypeStruct(a.shape, F32) for a in moments],
        in_specs=[vmem] * 4 + [hbm] * 6,
        out_specs=[hbm] * 9,
        scratch_shapes=[
            pltpu.VMEM((own, BLOCK, BLOCK), F32),
            *(pltpu.VMEM((OUTPUTS, PIECE, BLOCK), dtype) for dtype in (BF16, F32, F32)),
            pltpu.SemaphoreType.DMA((own,)),
            pltpu.SemaphoreType.DMA((OUTPUTS, 3)),
        ],
        compiler_params=pltpu.CompilerParams(vmem_limit_bytes=UPDATE_LIMIT),
        name="update",
    )(g, w, kept, wide, *moments)


def solution(mesh):
    def step(x, dy, *arrays):
        weights, moments = arrays[:3], arrays[3:]
        there = gradients(x, dy, weights, moments)
        there = [pltpu.with_memory_space_constraint(a, pltpu.VMEM) for a in there]
        moments = [pltpu.with_memory_space_constraint(a, pltpu.HBM) for a in moments]
        return tuple(update(*there, weights, moments))

    return jax.shard_map(
        step,
        mesh=mesh,
        in_specs=(P(("rep", "dp"), None, None),) * 2 + (P(None, None, None),) * 9,
        out_specs=(P("rep", None, None),) * 9,
        check_vma=False,
    )
```
